32 devices in a mesh: fsdp: 4 (over z), context: 4 (over y, x), tensor: 2 (over core).
Axes of the slice: x: 2, y: 2, z: 4, core: 2. Of those that a mesh axis runs over, the one named last changes fastest.
Arguments:
- hidden: bfloat16 [4, 512, 1024], P('fsdp', 'context'), may hold values from -6 to 6
- segments: int32 [4, 512], P('fsdp', 'context'), may hold values from 0 to 3, never falling along the last dimension, each value on 1 to 256 neighbouring positions
- w_query: bfloat16 [1024, 2048], P(('fsdp', 'context'), 'tensor'), may hold values from -0.1875 to 0.1875
- key_projection: bfloat16 [1024, 1024], P(('fsdp', 'context'), 'tensor'), may hold values from -0.1875 to 0.1875
- value_projection: bfloat16 [1024, 1024], P(('fsdp', 'context'), 'tensor'), may hold values from -0.1875 to 0.1875
- w_out: bfloat16 [2048, 1024], P('tensor', ('fsdp', 'context')), may hold values from -0.5 to 0.5
- w_gate: bfloat16 [1024, 3072], P(('fsdp', 'context'), 'tensor'), may hold values from -0.1875 to 0.1875
- w_up: bfloat16 [1024, 3072], P(('fsdp', 'context'), 'tensor'), may hold values from -0.1875 to 0.1875
- w_down: bfloat16 [3072, 1024], P('tensor', ('fsdp', 'context')), may hold values from -0.109375 to 0.109375
- gain_attn: bfloat16 [1024], P(('fsdp', 'context')), may hold values from 0.5 to 1.5
- gain_ffn: bfloat16 [1024], P(('fsdp', 'context')), may hold values from 0.5 to 1.5
- query_norm_gain: bfloat16 [128], P(('fsdp', 'context')), may hold values from 0.5 to 1.5
- gain_key: bfloat16 [128], P(('fsdp', 'context')), may hold values from 0.5 to 1.5
- cotangent: bfloat16 [4, 512, 1024], P('fsdp', 'context'), may hold values from -6 to 6
Outputs:
- output: bfloat16 [4, 512, 1024], P('fsdp', 'context')
- grad_hidden: bfloat16 [4, 512, 1024], P('fsdp', 'context')
- grad_w_query: float32 [1024, 2048], P(('fsdp', 'context'), 'tensor')
- grad_w_key: float32 [1024, 1024], P(('fsdp', 'context'), 'tensor')
- grad_w_value: float32 [1024, 1024], P(('fsdp', 'context'), 'tensor')
- grad_w_out: float32 [2048, 1024], P('tensor', ('fsdp', 'context'))
- grad_w_gate: float32 [1024, 3072], P(('fsdp', 'context'), 'tensor')
- grad_w_up: float32 [1024, 3072], P(('fsdp', 'context'), 'tensor')
- grad_w_down: float32 [3072, 1024], P('tensor', ('fsdp', 'context'))
- grad_gain_attn: float32 [1024], P(('fsdp', 'context'))
- grad_gain_ffn: float32 [1024], P(('fsdp', 'context'))
- grad_gain_query: float32 [128], P(('fsdp', 'context'))
- grad_gain_key: float32 [128], P(('fsdp', 'context'))
The draws below stay inside these ranges and needn't reach their ends.
Inputs may be any that keep to these rules, and one draw needn't show every extreme that they name: `segments`: within each sequence the document numbers start at 0 and never fall along the positions; each document holds at most 256 tokens, and one holds exactly 256.
All inputs are finite; a program needn't handle non-finite values.
Results may differ from the reference program's by a relative error of at most 0.023.
Values may be sent and summed in bfloat16 or wider, within the bound.
No kernel may reach another device: no remote copies, remote signals or barrier semaphores. Data moves between devices by JAX's collectives and lax.ppermute only.
A program may use at most 128 MiB of HBM per device.

```python
import math
import jax
import jax.numpy as jnp
import numpy as np
from jax import lax

MODEL_WIDTH = 1024
FF = 3072
QUERY_HEADS = 16
KEY_VALUE_HEADS = 8
HEAD_SIZE = 128
LENGTH = 512
SEQS = 4
MOST = 256
DOCS = 4


def steps_of(rng, extent, cuts, smallest, high):
    factor_of, own = 1.0, jax.random.fold_in(rng, 6)
    for dim, blocks in cuts:
        draws = jnp.exp(jax.random.uniform(jax.random.fold_in(own, dim), (blocks,), jnp.float32, smallest / len(cuts), high / len(cuts)))
        factor_of = factor_of * jnp.repeat(draws, extent[dim] // blocks).reshape([-1 if axis == dim else 1 for axis in range(len(extent))])
    return factor_of


def length_profile(count, total, reach, lean):
    portions = [(1 << 20) // math.isqrt(standing ** lean) + 1 for standing in range(2, count + 1)]
    surplus, counts = total - reach - (count - 1), [1] * (count - 1)
    while surplus > 0:
        candidates = [i for i in range(count - 1) if counts[i] < reach]
        whole, left = sum([portions[i] for i in candidates]), surplus
        for i in candidates:
            extra = min(reach - counts[i], max(1, left * portions[i] // whole), surplus)
            counts[i] = counts[i] + extra
            surplus = surplus - extra
    return np.array([reach] + counts)


def uneven_parts(own_key, amount, total, reach, lean):
    if amount == 2:
        one = jax.random.randint(own_key, (), max(1, total - reach), min(reach, total - 1) + 1)
        return jnp.stack([one, total - one])
    tallies = jnp.asarray(length_profile(amount, total, reach, lean), jnp.int32)
    twos = (amount - 1) // 2
    giver, sink = tallies[1:1 + 2 * twos:2], tallies[2:2 + 2 * twos:2]
    slack = jnp.minimum(giver - 1, reach - sink)
    shifted = jax.random.randint(jax.random.fold_in(own_key, 1), (twos,), 0, 1 << 20) % (slack + 1)
    tallies = tallies.at[1:1 + 2 * twos:2].set(giver - shifted).at[2:2 + 2 * twos:2].set(sink + shifted)
    return tallies[jax.random.permutation(jax.random.fold_in(own_key, 2), amount)]


def bell_draw(stream_key, extent, width, bound, split=(), kind=jnp.bfloat16):
    values = width * jax.random.normal(stream_key, extent, jnp.float32)
    if split:
        values = values * steps_of(stream_key, extent, split, -0.22, 0.18)
    return jnp.clip(values, -bound, bound).astype(kind)


def setup_inputs(seed: int = 0) -> dict:
    arg_keys = jax.random.split(jax.random.key(seed), 15)
    return {
        "hidden": bell_draw(arg_keys[0], (SEQS, LENGTH, MODEL_WIDTH), 1.0, 6.0, ((0, 4), (1, 4))),
        "segments": jax.vmap(lambda own: jnp.searchsorted(jnp.cumsum(uneven_parts(own, DOCS, LENGTH, MOST, 2)), jnp.arange(LENGTH), side="right"))(jax.random.split(arg_keys[1], SEQS)).reshape((SEQS, LENGTH)).astype(jnp.int32),
        "w_query": bell_draw(arg_keys[2], (MODEL_WIDTH, QUERY_HEADS * HEAD_SIZE), MODEL_WIDTH ** -0.5, 0.1875, ((0, 16), (1, 2))),
        "key_projection": bell_draw(arg_keys[3], (MODEL_WIDTH, KEY_VALUE_HEADS * HEAD_SIZE), MODEL_WIDTH ** -0.5, 0.1875, ((0, 16), (1, 2))),
        "value_projection": bell_draw(arg_keys[4], (MODEL_WIDTH, KEY_VALUE_HEADS * HEAD_SIZE), MODEL_WIDTH ** -0.5, 0.1875, ((0, 16), (1, 2))),
        "w_out": bell_draw(arg_keys[5], (QUERY_HEADS * HEAD_SIZE, MODEL_WIDTH), (QUERY_HEADS * HEAD_SIZE // 16) ** -0.5, 0.5, ((0, 2), (1, 16))),
        "w_gate": bell_draw(arg_keys[6], (MODEL_WIDTH, FF), MODEL_WIDTH ** -0.5, 0.1875, ((0, 16), (1, 2))),
        "w_up": bell_draw(arg_keys[7], (MODEL_WIDTH, FF), MODEL_WIDTH ** -0.5, 0.1875, ((0, 16), (1, 2))),
        "w_down": bell_draw(arg_keys[8], (FF, MODEL_WIDTH), FF ** -0.5, 0.109375, ((0, 2), (1, 16))),
        "gain_attn": jnp.clip(1.0 + 0.1 * jax.random.normal(arg_keys[9], (MODEL_WIDTH,), jnp.float32), 0.5, 1.5).astype(jnp.bfloat16),
        "gain_ffn": jnp.clip(1.0 + 0.1 * jax.random.normal(arg_keys[10], (MODEL_WIDTH,), jnp.float32), 0.5, 1.5).astype(jnp.bfloat16),
        "query_norm_gain": jnp.clip(1.0 + 0.1 * jax.random.normal(arg_keys[11], (HEAD_SIZE,), jnp.float32), 0.5, 1.5).astype(jnp.bfloat16),
        "gain_key": jnp.clip(1.0 + 0.1 * jax.random.normal(arg_keys[12], (HEAD_SIZE,), jnp.float32), 0.5, 1.5).astype(jnp.bfloat16),
        "cotangent": bell_draw(arg_keys[13], (SEQS, LENGTH, MODEL_WIDTH), 1.0, 6.0, ((0, 4), (1, 4))),
    }


@jax.custom_vjp
def lowered_input(v):
    return lax.optimization_barrier(v.astype(jnp.bfloat16)).astype(jnp.float32)

@jax.custom_vjp
def lowered_backward(v):
    return v

def low_keep(v):
    return (lowered_input(v), None)

def low_pass(kept, grad):
    return (grad,)

def back_keep(v):
    return (v, None)

def back_low(kept, grad):
    return (lowered_input(grad),)
lowered_input.defvjp(low_keep, low_pass)
lowered_backward.defvjp(back_keep, back_low)
epsilon = 1e-06
theta_base = 1000000.0

def matrix_product(left, right):
    return jnp.dot(left, right, precision=lax.Precision.HIGHEST, preferred_element_type=jnp.float32)

def row_normalize(values, gain):
    return values * lax.rsqrt(lax.optimization_barrier(jnp.mean(values * values, axis=-1, keepdims=True)) + epsilon) * gain

def rope_tables(count):
    half_width = HEAD_SIZE // 2
    freq = theta_base ** (-(jnp.arange(half_width, dtype=jnp.float32) * 2.0 / HEAD_SIZE))
    angle = jnp.arange(count, dtype=jnp.float32)[:, None] * freq[None, :]
    return (jnp.cos(angle), jnp.sin(angle))

def rotary_apply(values, cosine_table, sine_table):
    half_width = values.shape[-1] // 2
    first_half = values[..., :half_width]
    second_half = values[..., half_width:]
    cosine_table = cosine_table[:, None, :]
    sine_table = sine_table[:, None, :]
    return jnp.concatenate([first_half * cosine_table - second_half * sine_table, second_half * cosine_table + first_half * sine_table], axis=-1)

def attend(query, key_all, value_all, seg_all):
    length_total = query.shape[0]
    block = math.gcd(length_total, 512)
    blocks = length_total // block
    scale = HEAD_SIZE ** (-0.5)
    positions = jnp.arange(length_total, dtype=jnp.int32)
    query_blocks = query.reshape((blocks, block) + query.shape[1:])
    seg_blocks = seg_all.reshape(blocks, block)
    pos_blocks = positions.reshape(blocks, block)

    def one_block(item):
        query_part, seg_part, pos_part = item
        allowed = (seg_part[:, None] == seg_all[None, :]) & (pos_part[:, None] >= positions[None, :])
        scores = lowered_backward(jnp.einsum('qgrh,kgh->grqk', query_part, key_all, precision=lax.Precision.HIGHEST) * scale)
        expo = jnp.where(allowed, jnp.exp(scores), 0.0)
        totals = lax.optimization_barrier(jnp.sum(expo, axis=-1))
        numer = lowered_backward(jnp.einsum('grqk,kgh->qgrh', lowered_input(expo), value_all, precision=lax.Precision.HIGHEST))
        return numer / jnp.transpose(totals, (2, 0, 1))[..., None]
    result = lax.map(jax.checkpoint(one_block), (query_blocks, seg_blocks, pos_blocks))
    return result.reshape(length_total, QUERY_HEADS * HEAD_SIZE)

def forward(x_rows, seg_rows, w_query, key_projection, value_projection, w_out, w_gate, w_up, w_down, gain_attn, gain_ffn, query_norm_gain, gain_key):
    length_total = x_rows.shape[0]
    query_group = QUERY_HEADS // KEY_VALUE_HEADS
    hidden_lowered = lowered_input(row_normalize(x_rows, gain_attn))
    query_unrotated = lowered_backward(matrix_product(hidden_lowered, w_query)).reshape(length_total, QUERY_HEADS, HEAD_SIZE)
    key_unrotated = lowered_backward(matrix_product(hidden_lowered, key_projection)).reshape(length_total, KEY_VALUE_HEADS, HEAD_SIZE)
    value_lowered = lowered_input(lowered_backward(matrix_product(hidden_lowered, value_projection))).reshape(length_total, KEY_VALUE_HEADS, HEAD_SIZE)
    cosine_table, sine_table = rope_tables(length_total)
    query_lowered = lowered_input(rotary_apply(row_normalize(query_unrotated, query_norm_gain), cosine_table, sine_table)).reshape(length_total, KEY_VALUE_HEADS, query_group, HEAD_SIZE)
    key_low = lowered_input(rotary_apply(row_normalize(key_unrotated, gain_key), cosine_table, sine_table))
    attn_o = attend(query_lowered, key_low, value_lowered, seg_rows)
    x_mid = x_rows + lowered_backward(matrix_product(lowered_input(attn_o), w_out))
    h_two = lowered_input(row_normalize(x_mid, gain_ffn))
    gate = lowered_backward(matrix_product(h_two, w_gate))
    up_proj = lowered_backward(matrix_product(h_two, w_up))
    hidden_units = lowered_input(jax.nn.silu(gate) * up_proj)
    return x_mid + lowered_backward(matrix_product(hidden_units, w_down))

def reference(hidden, segments, w_query, key_projection, value_projection, w_out, w_gate, w_up, w_down, gain_attn, gain_ffn, query_norm_gain, gain_key, cotangent):
    weights = tuple((item.astype(jnp.float32) for item in (w_query, key_projection, value_projection, w_out, w_gate, w_up, w_down, gain_attn, gain_ffn, query_norm_gain, gain_key)))

    def per_sequence(totals, item):
        x_seq, seg_seq, cot_seq = item

        def run(x_in, *params):
            return forward(x_in, seg_seq, *params)
        result, pull = jax.vjp(run, x_seq.astype(jnp.float32), *weights)
        grads = pull(cot_seq.astype(jnp.float32))
        totals = tuple((left + right for left, right in zip(totals, grads[1:])))
        return (totals, (result.astype(jnp.bfloat16), grads[0].astype(jnp.bfloat16)))
    zeros = tuple((jnp.zeros(item.shape, jnp.float32) for item in weights))
    sums, (output, grad_hidden) = lax.scan(per_sequence, zeros, (hidden, segments, cotangent))
    return (output, grad_hidden, sums[0], sums[1], sums[2], sums[3], sums[4], sums[5], sums[6], sums[7], sums[8], sums[9], sums[10])
```

```python
import jax
import jax.numpy as jnp
from jax import lax
from jax.sharding import PartitionSpec as P

HEAD = 128
EPS = 1e-06
THETA = 1000000.0
BF = jnp.bfloat16
F32 = jnp.float32


def mm(a, b):
    return lax.dot_general(a, b, (((1,), (0,)), ((), ())), preferred_element_type=F32)


def mm_t(a, b):
    return lax.dot_general(a, b, (((1,), (1,)), ((), ())), preferred_element_type=F32)


def mt_m(a, b):
    return lax.dot_general(a, b, (((0,), (0,)), ((), ())), preferred_element_type=F32)


def norm_rows(v, g):
    r = lax.rsqrt(jnp.mean(v * v, axis=-1, keepdims=True) + EPS)
    return v * r * g, r


def norm_back(v, r, g, up):
    n = v * r
    w = up * g
    return r * (w - n * jnp.mean(w * n, axis=-1, keepdims=True)), up * n


def rope(v, cos, sin):
    a = v[..., : HEAD // 2]
    b = v[..., HEAD // 2 :]
    return jnp.concatenate([a * cos - b * sin, b * cos + a * sin], axis=-1)


def swap(x, axis, n, k):
    return lax.ppermute(x, axis, [(i, i ^ k) for i in range(n)])


def gather(x, axis, n):
    return [x] + [swap(x, axis, n, k) for k in range(1, n)]


def scatter(blocks, axis, n):
    return [blocks[0]] + [swap(blocks[k], axis, n, k) for k in range(1, n)]


def absolute(blocks, me, n):
    s = jnp.stack(blocks)
    return [lax.dynamic_index_in_dim(s, me ^ j, 0, keepdims=False) for j in range(n)]


def cols(w, start, width):
    return lax.dynamic_slice_in_dim(w, start, width, 1)


def lanes(v, width=128):
    return jnp.concatenate([v, jnp.zeros((width - v.shape[0],), v.dtype)])


def solution(mesh):
    F, C, T = mesh.shape["fsdp"], mesh.shape["context"], mesh.shape["tensor"]

    def local(
        hidden, segments, w_query, w_key, w_value, w_out, w_gate, w_up, w_down,
        gain_attn, gain_ffn, gain_query, gain_key, cotangent,
    ):
        f, c, t = lax.axis_index("fsdp"), lax.axis_index("context"), lax.axis_index("tensor")
        tokens, width = hidden.shape[1], hidden.shape[2]
        half = tokens // T
        rows = w_query.shape[0]
        grow = gain_query.shape[0]
        kv_local = w_key.shape[1] // HEAD
        qc = w_query.shape[1] // C
        kw = max(HEAD, w_key.shape[1] // C)
        hc = w_gate.shape[1] // F
        hp = -(-hc // 128) * 128
        qh, kh = qc // HEAD, kw // HEAD
        group = qh // kh
        aw = qc + 2 * kw
        R = T * C * half
        scale = HEAD ** (-0.5)

        def my_half(x):
            return lax.dynamic_slice_in_dim(x, t * half, half, 0)

        def swap_t(x):
            return swap(x, "tensor", T, 1)

        hid = hidden.reshape(tokens, width)
        x_half = my_half(hid)
        seg_half = my_half(segments.reshape(tokens)).astype(BF)
        seg_rows = jnp.zeros((8, width), BF).at[0, :half].set(seg_half)
        xs = jnp.stack(gather(jnp.concatenate([x_half, seg_rows], 0), "context", C))
        xs = jnp.stack([xs, swap_t(xs)])
        x_all = xs[:, :, :half].reshape(R, width).astype(F32)
        seg = xs[:, :, half, :half].reshape(R).astype(jnp.int32)

        gains = jnp.concatenate(
            [lanes(jnp.concatenate([gain_attn, gain_ffn])), lanes(gain_query), lanes(gain_key, aw - 256)]
        )
        gains = jnp.concatenate([gains[None], jnp.zeros((7, aw), BF)], 0)

        def attn_cols(d):
            ks = (d * kv_local // C) * HEAD
            return jnp.concatenate([cols(w_query, d * qc, qc), cols(w_key, ks, kw), cols(w_value, ks, kw)], 1)

        wq_parts = [jnp.concatenate([attn_cols(c ^ k), gains], 0) for k in range(C)]
        wq = jnp.stack(absolute(scatter(wq_parts, "context", C), c, C))
        wq = jnp.stack(absolute(gather(wq, "fsdp", F), f, F))
        g_rows = wq[:, :, rows].astype(F32)
        g_attn = g_rows[:, :, :rows].reshape(width)
        g_ffn = g_rows[:, :, rows : 2 * rows].reshape(width)
        g_q = g_rows[:, :, 128 : 128 + grow].reshape(HEAD)
        g_k = g_rows[:, :, 256 : 256 + grow].reshape(HEAD)
        w_qkv = wq[:, :, :rows].reshape(width, aw)
        wo_t = w_out.T
        wo = jnp.stack(absolute(scatter([cols(wo_t, (c ^ k) * qc, qc) for k in range(C)], "context", C), c, C))
        wo = jnp.stack(absolute(gather(wo, "fsdp", F), f, F)).reshape(width, qc)
        wd_t = w_down.T

        def ffn_cols(d):
            pad = jnp.zeros((rows, hp - hc), BF)
            return jnp.concatenate(sum([[cols(w, d * hc, hc), pad] for w in (w_gate, w_up, wd_t)], []), 1)

        wf = jnp.stack(absolute(scatter([ffn_cols(f ^ k) for k in range(F)], "fsdp", F), f, F))
        wf = jnp.stack(absolute(gather(wf, "context", C), c, C), 1).reshape(width, 3 * hp)
        wg, wu, wd = wf[:, :hp], wf[:, hp : 2 * hp], wf[:, 2 * hp :]

        idx = jnp.arange(R, dtype=jnp.int32)
        trel, k, i = idx // (C * half), (idx // half) % C, idx % half
        pos = (c ^ k) * tokens + (t ^ trel) * half + i
        freq = THETA ** (-(jnp.arange(HEAD // 2, dtype=F32) * 2.0 / HEAD))
        angle = pos.astype(F32)[:, None] * freq[None, :]
        cos, sin = jnp.cos(angle), jnp.sin(angle)
        allowed = (seg[:, None] == seg[None, :]) & (pos[:, None] >= pos[None, :])

        def head(x, j):
            return x[:, j * HEAD : (j + 1) * HEAD]

        def reduce(part, axis, n):
            own = part[: R // 2] + swap_t(part[R // 2 :].astype(BF)).astype(F32)
            own = own.reshape(n, half, width)
            got = scatter([own[0]] + [own[j].astype(BF) for j in range(1, n)], axis, n)
            return sum([b.astype(F32) for b in got])

        def spread(x, axis, n):
            s = jnp.stack(gather(x, axis, n))
            return jnp.stack([s, swap_t(s)]).reshape(R, width)

        def both_halves(x):
            y = swap_t(x)
            return jnp.where(t == 0, jnp.concatenate([x, y], 0), jnp.concatenate([y, x], 0))

        dy = spread(my_half(cotangent.reshape(tokens, width)), "fsdp", F)

        h, r1 = norm_rows(x_all, g_attn)
        h = h.astype(BF)
        raw = mm(h, w_qkv)
        q_raw = [head(raw, j) for j in range(qh)]
        k_raw = [head(raw, qh + j) for j in range(kh)]
        v = [head(raw, qh + kh + j).astype(BF) for j in range(kh)]
        qn = [norm_rows(a, g_q) for a in q_raw]
        kn = [norm_rows(a, g_k) for a in k_raw]
        q = [rope(a, cos, sin).astype(BF) for a, _ in qn]
        ky = [rope(a, cos, sin).astype(BF) for a, _ in kn]
        ex, tot, at = [], [], []
        for j in range(qh):
            s = mm_t(q[j], ky[j // group]) * scale
            e = jnp.where(allowed, jnp.exp(s), 0.0)
            total = jnp.sum(e, -1, keepdims=True)
            ex.append(e)
            tot.append(total)
            at.append(mm(e.astype(BF), v[j // group]) / total)
        o = jnp.concatenate([a.astype(BF) for a in at], 1)
        branch = reduce(mm_t(o, wo), "context", C)
        x_mid = x_half.astype(F32) + branch
        h2h, r2 = norm_rows(x_mid, g_ffn)
        h2 = spread(h2h.astype(BF), "fsdp", F)

        gate, up = mm(h2, wg), mm(h2, wu)
        sg = jax.nn.sigmoid(gate)
        u = (gate * sg * up).astype(BF)
        du = mm(dy, wd)
        d_gate = (du * up * sg * (1.0 + gate * (1.0 - sg))).astype(BF)
        d_up = (du * gate * sg).astype(BF)
        dh2 = reduce(mm_t(d_gate, wg) + mm_t(d_up, wu), "fsdp", F)
        out = (x_mid + reduce(mm_t(u, wd), "fsdp", F)).astype(BF)
        gf = jnp.concatenate([mt_m(h2, d_gate), mt_m(h2, d_up), mt_m(dy, u)], 1).astype(BF)
        gf = gf.reshape(F, C, rows, 3 * hp)
        gf = scatter([lax.dynamic_index_in_dim(gf, c ^ j, 1, keepdims=False) for j in range(C)], "context", C)
        gf = sum([b.astype(F32) for b in gf]).astype(BF)
        gf = scatter([lax.dynamic_index_in_dim(gf, f ^ j, 0, keepdims=False) for j in range(F)], "fsdp", F)
        gf = jnp.stack(absolute(gf, f, F), 1).astype(F32)
        ffn_grads = [gf[:, :, j * hp : j * hp + hc].reshape(rows, F * hc) for j in range(3)]

        inward, gn_rows = norm_back(x_mid, r2, g_ffn, dh2)
        dg_ffn = jnp.sum(gn_rows, 0)
        dx_mid = my_half(cotangent.reshape(tokens, width)).astype(F32) + inward
        dx = spread(dx_mid.astype(BF), "context", C)

        g_o = mt_m(dx, o).astype(BF)
        g_att = mm(dx, wo)
        dq, dk, dv = [], [0.0] * kh, [0.0] * kh
        for j in range(qh):
            g = head(g_att, j)
            gs = (g / tot[j]).astype(BF)
            dt = -jnp.sum(g * at[j], -1, keepdims=True) / tot[j]
            dv[j // group] += mt_m(ex[j].astype(BF), gs)
            ds = (ex[j] * (mm_t(gs, v[j // group]) + dt)).astype(BF)
            dq.append(mm(ds, ky[j // group]) * scale)
            dk[j // group] += mt_m(ds, q[j]) * scale
        dgq, dgk, draw = 0.0, 0.0, []
        for j in range(qh):
            a, b = norm_back(q_raw[j], qn[j][1], g_q, rope(dq[j], cos, -sin))
            draw.append(a.astype(BF))
            dgq += jnp.sum(b, 0)
        for j in range(kh):
            a, b = norm_back(k_raw[j], kn[j][1], g_k, rope(dk[j], cos, -sin))
            draw.append(a.astype(BF))
            dgk += jnp.sum(b, 0)
        draw = jnp.concatenate(draw + [a.astype(BF) for a in dv], 1)
        dh_part = mm_t(draw, w_qkv)
        dg_attn = jnp.sum(dh_part * (x_all * r1), 0)
        gq = mt_m(h, draw).reshape(F, C, rows, aw)
        extra = jnp.concatenate(
            [
                dg_attn.reshape(F, C, rows), dg_ffn.reshape(F, C, rows),
                jnp.zeros((F, C, 128 - 2 * rows), F32),
                dgq.reshape(F, C, grow), jnp.zeros((F, C, 128 - grow), F32),
                dgk.reshape(F, C, grow), jnp.zeros((F, C, aw - 256 - grow), F32),
            ],
            2,
        )[:, :, None]
        gq = jnp.concatenate([gq, extra, jnp.zeros((F, C, 7, aw), F32)], 2).astype(BF)

        def to_owner(g):
            g = scatter([lax.dynamic_index_in_dim(g, f ^ j, 0, keepdims=False) for j in range(F)], "fsdp", F)
            g = sum([b.astype(F32) for b in g]).astype(BF)
            g = scatter([lax.dynamic_index_in_dim(g, c ^ j, 0, keepdims=False) for j in range(C)], "context", C)
            return jnp.stack(absolute(g, c, C)).astype(F32)

        gq = to_owner(gq)
        go = to_owner(g_o.reshape(F, C, rows, qc))
        dh = reduce(dh_part, "context", C)
        inward, _ = norm_back(x_half.astype(F32), lax.rsqrt(jnp.mean(x_half.astype(F32) ** 2, -1, keepdims=True) + EPS), g_attn, dh)
        grad_hidden = (dx_mid + inward).astype(BF)

        ge = jnp.sum(gq[:, rows], 0)
        ge = ge + swap_t(ge)
        share = kw * C // w_key.shape[1]
        gq = jnp.swapaxes(gq[:, :rows], 0, 1)

        def kv_grad(g):
            return g.reshape(rows, C // share, share, kw).sum(2).reshape(rows, w_key.shape[1])

        return (
            both_halves(out).reshape(1, tokens, width),
            both_halves(grad_hidden).reshape(1, tokens, width),
            gq[:, :, :qc].reshape(rows, C * qc),
            kv_grad(gq[:, :, qc : qc + kw]),
            kv_grad(gq[:, :, qc + kw :]),
            jnp.swapaxes(go, 0, 1).reshape(rows, C * qc).T,
            ffn_grads[0], ffn_grads[1], ffn_grads[2].T,
            ge[:rows], ge[rows : 2 * rows], ge[128 : 128 + grow], ge[256 : 256 + grow],
        )

    both = ("fsdp", "context")
    seq, row, col, vec = P("fsdp", "context", None), P(both, "tensor"), P("tensor", both), P(both)
    return jax.shard_map(
        local,
        mesh=mesh,
        in_specs=(seq, P("fsdp", "context"), row, row, row, col, row, row, col, vec, vec, vec, vec, seq),
        out_specs=(seq, seq, row, row, row, col, row, row, col, vec, vec, vec, vec),
        check_vma=False,
    )
```

```python
import jax
import jax.numpy as jnp
from jax import lax
from jax.experimental import pallas as pl
from jax.experimental.pallas import tpu as pltpu
from jax.sharding import PartitionSpec as P

HEAD = 128
EPS = 1e-06
THETA = 1000000.0
BF = jnp.bfloat16
F32 = jnp.float32


def mm(a, b):
    return lax.dot_general(a, b, (((1,), (0,)), ((), ())), preferred_element_type=F32)


def mm_t(a, b):
    return lax.dot_general(a, b, (((1,), (1,)), ((), ())), preferred_element_type=F32)


def mt_m(a, b):
    return lax.dot_general(a, b, (((0,), (0,)), ((), ())), preferred_element_type=F32)


def inv_rms(v):
    return lax.rsqrt(jnp.mean(v * v, axis=-1, keepdims=True) + EPS)


def norm_back(v, r, g, up):
    n = v * r
    w = up * g
    return r * (w - n * jnp.mean(w * n, axis=-1, keepdims=True)), up * n


def swap(x, axis, n, k):
    return lax.ppermute(x, axis, [(i, i ^ k) for i in range(n)])


def bits(n):
    return n.bit_length() - 1


def turned(j, n):
    return sum(((j >> i) & 1) << (bits(n) - 1 - i) for i in range(bits(n)))


def mask_of(j, n, t):
    return j + t * (turned(j, n) - j)


def hop(x, axis, n, i):
    steps = [1 << i, 1 << (bits(n) - 1 - i)]
    return lax.ppermute(x, (axis, "tensor"), [(2 * d + t, 2 * (d ^ steps[t]) + t) for d in range(n) for t in range(2)])


def scatter(blocks, axis, n):
    got = {k: swap(blocks[k], axis, n, k) for k in range(n - 1, 0, -1)}
    return [blocks[0]] + [got[k] for k in range(1, n)]


def join(a, b):
    def body(a_ref, b_ref, o_ref):
        o_ref[: a.shape[0]] = a_ref[...]
        o_ref[a.shape[0] :] = b_ref[...]

    return call(body, [shape(2 * a.shape[0], *a.shape[1:])], [a, b], vmem_mb=8)[0]


def gather(x, axis, n):
    x = x[None]
    for i in range(bits(n)):
        got = hop(x, axis, n, i)
        if i < bits(n) - 1:
            x = join(x, got)
    return [x, got]


def reduce_blocks(low, high, axis, n, gate=None, first=None):
    for i in range(bits(n) - 1, -1, -1):
        got = hop(high, axis, n, i)
        if first is not None and i == bits(n) - 1:
            first.append(got)
        if gate is not None and i:
            got = after(got, gate)
        low = low.astype(F32) + got.astype(F32)
        if i:
            keep = low.shape[0] // 2
            low, high = low[:keep], low[keep:].astype(BF)
    return low[0]


def after(x, *deps):
    return lax.optimization_barrier((x, deps))[0]


def at(offset, size, unit):
    return pl.ds(pl.multiple_of(offset, unit), size)


def call(body, outs, args, scratch=(), flops=0, vmem_mb=20, hbm=0, hbm_outs=0):
    vmem = pl.BlockSpec(memory_space=pltpu.VMEM)
    far = pl.BlockSpec(memory_space=pltpu.MemorySpace.HBM)
    moved = sum(a.size * a.dtype.itemsize for a in list(args) + list(outs))
    return pl.pallas_call(
        body,
        out_shape=list(outs),
        in_specs=[far] * hbm + [vmem] * (len(args) - hbm),
        out_specs=[far] * hbm_outs + [vmem] * (len(outs) - hbm_outs),
        scratch_shapes=list(scratch),
        cost_estimate=pl.CostEstimate(flops=flops, bytes_accessed=moved, transcendentals=0),
        compiler_params=pltpu.CompilerParams(vmem_limit_bytes=vmem_mb * 1024 * 1024),
    )(*args)


def shape(*s, dtype=BF):
    return jax.ShapeDtypeStruct(s, dtype)


def solution(mesh):
    F, C, T = mesh.shape["fsdp"], mesh.shape["context"], mesh.shape["tensor"]

    def local(
        hidden, segments, w_query, w_key, w_value, w_out, w_gate, w_up, w_down,
        gain_attn, gain_ffn, gain_query, gain_key, cotangent,
    ):
        f, c, t = lax.axis_index("fsdp"), lax.axis_index("context"), lax.axis_index("tensor")
        tokens, width = hidden.shape[1], hidden.shape[2]
        half = tokens // T
        rows = w_query.shape[0]
        grow = gain_query.shape[0]
        kv_local = w_key.shape[1] // HEAD
        qc = w_query.shape[1] // C
        kw = max(HEAD, w_key.shape[1] // C)
        hc = w_gate.shape[1] // F
        hp = -(-hc // 128) * 128
        qh, kh = qc // HEAD, kw // HEAD
        group = qh // kh
        aw = qc + 2 * kw
        CR = C * rows
        R = T * C * half
        H = R // 2
        scale = HEAD ** (-0.5)
        share = kw * C // w_key.shape[1]
        wide = aw + qc + width
        CH, FH = C // 2, F // 2

        lane = (f * C + c) * rows % 128
        goff = (f * C + c) * grow

        hid = hidden.reshape(tokens, width)
        tall = max(rows, half)

        def me():
            return lax.axis_index("fsdp"), lax.axis_index("context")

        def ffn_pack(wg_ref, wu_ref, wd_ref, *refs):
            outs, sem = refs[:F], refs[F]
            mf, _ = me()
            copies = []
            for k in range(F):
                for j, w in enumerate((wg_ref, wu_ref, wd_ref)):
                    copies.append(pltpu.make_async_copy(w.at[:, at((mf ^ k) * hp, hp, 128)], outs[k].at[:, j * hp : (j + 1) * hp], sem.at[k, j]))
            for cp in copies:
                cp.start()
            for cp in copies:
                cp.wait()

        w_down = w_down.T
        if hp > hc:
            fill = [((0, 0), (0, 0), (0, hp - hc))]
            w_gate, w_up, w_down = [jnp.pad(w.reshape(rows, F, hc), *fill).reshape(rows, F * hp) for w in (w_gate, w_up, w_down)]
        wf = call(
            ffn_pack,
            [shape(rows, 3 * hp)] * F,
            [w_gate, w_up, w_down],
            [pltpu.SemaphoreType.DMA((F, 3))],
            hbm=3,
            vmem_mb=60,
        )
        def attn_pack(wq_ref, wk_ref, wv_ref, wo_ref, x_ref, ga_ref, gf_ref, gq_ref, gk_ref, s_ref, *refs):
            outs, sem = refs[:C], refs[C]
            mt = lax.axis_index("tensor")
            mf, mc = me()
            copies = []
            for k in range(C):
                d = mc ^ k
                ks = at(d * kv_local // C * HEAD, kw, 128)
                qs = at(d * qc, qc, 128)
                parts = [(wq_ref, qs, 0, qc), (wk_ref, ks, qc, kw), (wv_ref, ks, qc + kw, kw), (wo_ref, qs, aw, qc)]
                copies.append(pltpu.make_async_copy(x_ref.at[at(mt * half, half, half), :], outs[k].at[0:half, aw + qc :], sem.at[k, 4]))
                for m, (w, src, start, size) in enumerate(parts):
                    copies.append(pltpu.make_async_copy(w.at[:, src], outs[k].at[0:rows, start : start + size], sem.at[k, m]))
            for cp in copies:
                cp.start()
            dest = mf * C + mc
            lanes = lax.broadcasted_iota(jnp.int32, (8, 128), 1)
            docs = jnp.broadcast_to(s_ref[...].astype(F32), (8, 128))
            docs = jnp.where((lanes < half) == (mt == 0), docs, pltpu.roll(docs, half, 1))

            def placed(ref, want):
                size = ref.shape[1]
                r = lax.broadcasted_iota(jnp.int32, (size, 128), 0)
                pick = (lax.broadcasted_iota(jnp.int32, (size, 128), 1) == r + want).astype(F32).astype(BF)
                return mm(jnp.broadcast_to(ref[...].astype(F32), (8, size)).astype(BF), pick)[0:1]

            ln, hd = dest * rows % 128, dest * grow
            blank = jnp.zeros((1, aw - 384), F32) if aw > 384 else None
            first = [placed(ga_ref, ln), placed(gf_ref, ln), placed(gq_ref, hd)]
            first = jnp.concatenate(first + ([blank] if aw > 384 else []), 1)
            second = jnp.concatenate([placed(gk_ref, hd), jnp.zeros((1, aw - 128), F32)], 1)
            ext = jnp.concatenate([first, second, jnp.zeros((6, aw), F32)], 0).astype(BF)
            for k in range(C):
                outs[k][tall:, :aw] = ext
                outs[k][tall:, aw : aw + qc] = jnp.zeros((8, qc), BF)
                outs[k][tall:, aw + qc : aw + qc + 128] = docs.astype(BF)
                outs[k][tall:, aw + qc + 128 :] = jnp.zeros((8, width - 128), BF)
            for cp in copies:
                cp.wait()

        wa = call(
            attn_pack,
            [shape(tall + 8, wide)] * C,
            list(after((w_query, w_key, w_value, w_out.T, hid), wf[0]))
            + [v.reshape(1, -1) for v in (gain_attn, gain_ffn, gain_query, gain_key)]
            + [segments.reshape(1, tokens)],
            [pltpu.SemaphoreType.DMA((C, 5))],
            hbm=5,
            vmem_mb=60,
        )
        wa_got = scatter(wa, "context", C)

        wf = scatter(wf, "fsdp", F)

        def ffn_join(*refs):
            for k in range(F):
                refs[F][k] = refs[k][...]

        wf_got = wf
        wf = call(ffn_join, [shape(F, rows, 3 * hp)], [after(wf[0], wa_got[1])] + wf[1:], vmem_mb=8)[0]
        wf_first = hop(wf[None], "context", C, 0)
        wf_here = wf[None]

        def attn_join(*refs):
            b, qkv, o, x, docs = refs[:C], refs[C], refs[C + 1], refs[C + 2], refs[C + 3]
            mt = lax.axis_index("tensor")
            docs[...] = jnp.zeros_like(docs)
            for k in range(C):
                j = mask_of(k, C, mt)
                qkv[k * rows : (k + 1) * rows, :] = b[k][0:rows, :aw]
                o[k * rows : (k + 1) * rows, :] = b[k][0:rows, aw : aw + qc]
                x[at(j * half, half, half), :] = b[k][0:half, aw + qc :]
                docs[pl.ds(j, 1), :] = b[k][tall:, aw + qc : aw + qc + 128].astype(F32)[0:1]
            x[C * half :, :128] = docs[...].astype(BF)
            x[C * half :, 128:] = jnp.zeros((8, width - 128), BF)
            qkv[CR:, :] = jnp.concatenate([b[k][tall:, :aw].astype(F32)[0:2] for k in range(C)], 0).astype(BF)

        wq, wo, x_own = call(
            attn_join,
            [shape(CR + 2 * C, aw), shape(CR, qc), shape(C * half + 8, width)],
            [after(wa_got[0], wf_got)] + wa_got[1:],
            [pltpu.VMEM((8, 128), F32)],
        )
        wq = gather(wq, "fsdp", F)
        wo = gather(after(wo, wq[0]), "fsdp", F)

        def my_half(x):
            return lax.dynamic_slice_in_dim(x, t * half, half, 0)

        def other_half(x):
            return lax.dynamic_slice_in_dim(x, (1 - t) * half, half, 0)

        def swap_t(x):
            return swap(x, "tensor", T, 1)

        x_half = my_half(hid)
        xs = [x_own, swap_t(x_own)]

        idx = jnp.arange(R, dtype=jnp.int32)
        trel, k, i = idx // (C * half), (idx // half) % C, idx % half
        pos = (c ^ mask_of(k, C, t ^ trel)) * tokens + (t ^ trel) * half + i
        freq = THETA ** (-(jnp.arange(HEAD // 2, dtype=F32) * 2.0 / HEAD))
        angle = pos.astype(F32)[:, None] * freq[None, :]
        cos, sin = jnp.cos(angle), jnp.sin(angle)
        cos, sin = jnp.concatenate([cos, cos], 1), jnp.concatenate([-sin, sin], 1)
        pos_row = jnp.broadcast_to(pos[None], (8, R))
        pos_col = jnp.broadcast_to(pos[:, None], (R, 128))

        def find_allowed(a_ref, b_ref, pr_ref, pc_ref, out):
            copies = CH * (2 * half // 128)
            row = []
            for ref in (a_ref, b_ref):
                d = ref[C * half :, :128].astype(F32)
                d = jnp.concatenate([d] * (C * half // 128), 1)
                keep = lax.broadcasted_iota(jnp.int32, d.shape, 1) // half == lax.broadcasted_iota(jnp.int32, d.shape, 0)
                row.append(jnp.sum(jnp.where(keep, d, 0.0), 0, keepdims=True))
            row = jnp.broadcast_to(jnp.concatenate(row, 1), (8, R))
            first = (lax.broadcasted_iota(jnp.int32, (8, 128), 0) == 0).astype(F32).astype(BF)
            col = mt_m(row.astype(BF), first)
            pc = pc_ref[...]
            for m in range(R // 128):
                sl = slice(m * 128, (m + 1) * 128)
                ok = (col == row[0:1, sl]) & (pc >= pr_ref[0:1, sl])
                out[:, sl] = jnp.where(ok, 1.0, 0.0).astype(BF)

        allowed = call(find_allowed, [shape(R, R)], xs + [pos_row, pos_col])[0]

        def reduce(own, low, high, axis, n, gate=None, enter=None, first=None):
            keep = H // 2
            if high is None:
                low = swap_t(low)
                low, high = low[:keep], low[keep:]
            else:
                low, high = swap_t(low), swap_t(high)
            high = (own[keep:] + high.astype(F32)).astype(BF)
            low = own[:keep] + low.astype(F32)
            if enter is not None:
                high = after(high, enter)
            shaped = (n // 2, half, width)
            return reduce_blocks(low.reshape(shaped), high.reshape(shaped), axis, n, gate, first), high

        def spread(x, axis, n):
            b = [x]
            for i in range(bits(n)):
                b = b + [hop(a, axis, n, i) for a in b]
            return b + [swap_t(a) for a in b]

        def both_halves(x):
            y = swap_t(x)
            return jnp.where(t == 0, jnp.concatenate([x, y], 0), jnp.concatenate([y, x], 0))

        cot = cotangent.reshape(tokens, width)
        dys = gather(after(my_half(cot), wo[0]), "fsdp", F)
        dys = dys + [swap_t(b) for b in dys]

        def rotate(v, cs, sn):
            return v * cs + pltpu.roll(v, HEAD // 2, 1) * sn

        def split_rows(p, own, low, high):
            own[...] = p[:H]
            low[...] = p[H : H + H // 2].astype(BF)
            high[...] = p[H + H // 2 :].astype(BF)

        def split_whole(p, own, send):
            own[...] = p[:H]
            send[...] = p[H:].astype(BF)

        whole = [shape(H, width, dtype=F32), shape(H, width)]
        halves = [shape(H, width, dtype=F32), shape(H // 2, width), shape(H // 2, width)]

        got = wf_first
        for i in range(1, bits(C)):
            wf_here = join(wf_here, got)
            got = hop(wf_here, "context", C, i)
        wf = [wf_here, got]

        def attn_fwd(*refs):
            xb, wb, refs = refs[:2], refs[2:4], refs[4:]
            cs_ref, sn_ref, ok_ref = refs[:3]
            outs, o, gv, gqk = refs[3:9], refs[9], refs[10], refs[11]
            h, raw, q, ky, v, w = refs[12:18]
            sem = refs[18]
            mf, mc = me()
            mt = lax.axis_index("tensor")
            sent = [pltpu.make_async_copy(a, b, sem.at[m]) for m, (a, b) in enumerate(zip((h, raw, q, ky, v, w), outs))]
            gv[...] = jnp.zeros_like(gv)
            acc = jnp.zeros((2, 128), F32)
            for a in range(F):
                wa_ref = wb[a // FH]
                e = wa_ref[a % FH, CR:, :].astype(F32)
                for b in range(C):
                    dest = (mf ^ mask_of(a, F, mt)) * C + (mc ^ b)
                    w[at(dest * rows, rows, rows), :] = wa_ref[a % FH, b * rows : (b + 1) * rows, :]
                    blk = at(dest * rows // 128 * 128, 128, 128)
                    gv[0:1, blk] += e[2 * b : 2 * b + 1, 0:128]
                    gv[1:2, blk] += e[2 * b : 2 * b + 1, 128:256]
                    acc += jnp.concatenate([e[2 * b : 2 * b + 1, 256:384], e[2 * b + 1 : 2 * b + 2, 0:128]], 0)
            gqk[0:2, :] = acc
            g = gv[0:1, :]
            for b in range(2 * C):
                x = xb[b // C][b % C * half : (b % C + 1) * half, :].astype(F32)
                h[b * half : (b + 1) * half, :] = (x * inv_rms(x) * g).astype(BF)
            sent[0].start()
            sent[5].start()
            p = mm(h[...], w[...])
            raw[...] = p[:, : qc + kw]
            v[...] = p[:, qc + kw :].astype(BF)
            sent[1].start()
            sent[4].start()
            cs, sn = cs_ref[...], sn_ref[...]
            for j in range(qh + kh):
                a = p[:, j * HEAD : (j + 1) * HEAD]
                gg = gqk[0:1, :] if j < qh else gqk[1:2, :]
                rot = rotate(a * inv_rms(a) * gg, cs, sn).astype(BF)
                if j < qh:
                    q[:, j * HEAD : (j + 1) * HEAD] = rot
                else:
                    ky[:, (j - qh) * HEAD : (j - qh + 1) * HEAD] = rot
            sent[2].start()
            sent[3].start()
            ok = ok_ref[...].astype(F32) > 0.5
            for j in range(qh):
                qs = slice(j * HEAD, (j + 1) * HEAD)
                ks = slice(j // group * HEAD, (j // group + 1) * HEAD)
                e = jnp.where(ok, jnp.exp(mm_t(q[:, qs], ky[:, ks]) * scale), 0.0)
                o[:, qs] = (mm(e.astype(BF), v[:, ks]) / jnp.sum(e, -1, keepdims=True)).astype(BF)
            for cp in sent:
                cp.wait()

        kept = [shape(R, width), shape(R, qc + kw, dtype=F32), shape(R, qc), shape(R, kw), shape(R, kw), shape(width, aw)]
        h, raw, q, ky, v, w_qkv, o, gv, gqk = call(
            attn_fwd,
            kept + [shape(R, qc), shape(8, width, dtype=F32), shape(8, 128, dtype=F32)],
            xs + wq + [cos, sin, after(allowed, wf_first)],
            [pltpu.VMEM(a.shape, a.dtype) for a in kept] + [pltpu.SemaphoreType.DMA((6,))],
            flops=2 * R * width * aw + 4 * R * R * qc,
            hbm_outs=6,
        )

        def out_proj(o_ref, *refs):
            wb, own, low, high, w = refs[:2], *refs[2:]
            mf, mc = me()
            mt = lax.axis_index("tensor")
            for a in range(F):
                for b in range(C):
                    dest = (mf ^ mask_of(a, F, mt)) * C + (mc ^ b)
                    w[at(dest * rows, rows, rows), :] = wb[a // FH][a % FH, b * rows : (b + 1) * rows, :]
            split_rows(mm_t(o_ref[...], w[...]), own, low, high)

        res = call(
            out_proj,
            halves + [shape(width, qc)],
            [after(o, wf[1])] + wo,
            flops=2 * R * width * qc,
        )
        w_o = res[3]
        x_mid = x_half.astype(F32) + reduce(*res[:3], "context", C)[0]
        r2 = inv_rms(x_mid)
        g_ffn = gv[1:2]
        h2s = spread((x_mid * r2 * g_ffn).astype(BF), "fsdp", F)

        def ffn_pre(*refs):
            wb, db, w, dy, du = refs[:2], refs[2:6], *refs[6:]
            mf, mc = me()
            mt = lax.axis_index("tensor")
            for a in range(C):
                for b in range(F):
                    dest = (mf ^ b) * C + (mc ^ mask_of(a, C, mt))
                    w[at(dest * rows, rows, rows), :] = wb[a // CH][a % CH, b]
            for b in range(2 * F):
                dy[b * half : (b + 1) * half, :] = db[b // FH][b % FH]
            du[...] = mm(dy[...], w[:, 2 * hp :])

        w_f, dy, du = call(
            ffn_pre,
            [shape(width, 3 * hp), shape(R, width), shape(R, hp, dtype=F32)],
            wf + dys,
            flops=2 * R * width * hp,
        )

        def ffn_main(*refs):
            hb, w, du_ref, own, low, high, h2, act = refs[: 2 * F], *refs[2 * F :]
            for b in range(2 * F):
                h2[b * half : (b + 1) * half, :] = hb[b][...]
            p = mm(h2[...], w[:, : 2 * hp])
            gate, up = p[:, :hp], p[:, hp:]
            sg = 1.0 / (1.0 + jnp.exp(-gate))
            d = du_ref[...]
            sl = gate * sg
            act[:, :hp] = (d * up * sg * (1.0 + gate * (1.0 - sg))).astype(BF)
            act[:, hp : 2 * hp] = (d * sl).astype(BF)
            act[:, 2 * hp :] = (sl * up).astype(BF)
            split_rows(mm_t(act[:, : 2 * hp], w[:, : 2 * hp]), own, low, high)

        res = call(
            ffn_main,
            halves + [shape(R, width), shape(R, 3 * hp)],
            h2s + [w_f, du],
            flops=8 * R * width * hp,
        )
        h2, act = res[3:]
        dh2, dh2_sent = reduce(*res[:3], "fsdp", F)
        act = after(act, dh2_sent)

        def ffn_post(h2_ref, dy_ref, act_ref, w, *refs):
            own, send, gd, gu, g = refs[0], refs[1], refs[2:4], refs[4:6], refs[6]
            mf, mc = me()
            mt = lax.axis_index("tensor")
            g[:, : 2 * hp] = mt_m(h2_ref[...], act_ref[:, : 2 * hp]).astype(BF)
            g[:, 2 * hp :] = mt_m(dy_ref[...], act_ref[:, 2 * hp :]).astype(BF)
            for a in range(C):
                for b in range(F):
                    dest = (mf ^ b) * C + (mc ^ mask_of(a, C, mt))
                    src = at(dest * rows, rows, rows)
                    gu[a // CH][a % CH, b] = g[src, : 2 * hp]
                    gd[a // CH][a % CH, b] = g[src, 2 * hp :]
            split_whole(mm_t(act_ref[:, 2 * hp :], w[:, 2 * hp :]), own, send)

        res = call(
            ffn_post,
            whole + [shape(CH, F, rows, hp)] * 2 + [shape(CH, F, rows, 2 * hp)] * 2,
            [h2, dy, act, w_f],
            [pltpu.VMEM((width, 3 * hp), BF)],
            flops=8 * R * width * hp,
        )
        out_parts, down_parts, units_parts = list(res[:2]) + [None], res[2:4], res[4:6]

        inward, gn_rows = norm_back(x_mid, r2, g_ffn, dh2)
        dg_ffn = jnp.sum(gn_rows, 0, keepdims=True)
        dx_mid = my_half(cot).astype(F32) + inward
        dx_low = dx_mid.astype(BF)
        dxs = spread(dx_low, "context", C)
        units_first, out_first = [], []
        g_units = reduce_blocks(*after(units_parts, dxs[1:C]), "context", C, first=units_first)
        out = (x_mid + reduce(*out_parts, "fsdp", F, enter=dx_low, first=out_first)[0]).astype(BF)

        def out_back(*refs):
            db, o_ref, w, dx, ga, gb, g = refs[: 2 * C], *refs[2 * C : 2 * C + 4], refs[2 * C + 4 : -1], refs[-1]
            mf, mc = me()
            mt = lax.axis_index("tensor")
            for b in range(2 * C):
                dx[b * half : (b + 1) * half, :] = db[b][...]
            g[...] = mt_m(dx[...], o_ref[...]).astype(BF)
            for a in range(F):
                for b in range(C):
                    dest = (mf ^ mask_of(a, F, mt)) * C + (mc ^ b)
                    gb[a // FH][a % FH, b * rows : (b + 1) * rows, :] = g[at(dest * rows, rows, rows), :]
            ga[...] = mm(dx[...], w[...])

        res = call(
            out_back,
            [shape(R, width), shape(R, qc, dtype=F32)] + [shape(FH, CR, qc)] * 2,
            dxs + [o, w_o],
            [pltpu.VMEM((width, qc), BF)],
            flops=4 * R * width * qc,
        )
        o_first = []
        g_att, go = after(res[1], out_first[0]), reduce_blocks(*res[2:], "fsdp", F, first=o_first)
        g_down = reduce_blocks(*down_parts, "context", C, gate=res[1])

        def attn_back(*refs):
            xb, refs = refs[:2], refs[2:]
            ga, h_ref, raw, q, ky, v, w, gv_ref, gqk_ref, cs_ref, sn_ref, ok_ref, dgf, own, send = refs[:15]
            gb, draw, gs_ref, ex, gn = refs[15:17], *refs[17:]
            mf, mc = me()
            mt = lax.axis_index("tensor")
            cs, sn = cs_ref[...], sn_ref[...]
            ok = ok_ref[...].astype(F32) > 0.5
            dk, dv = [0.0] * kh, [0.0] * kh
            dgq, dgk = jnp.zeros((1, HEAD), F32), jnp.zeros((1, HEAD), F32)
            for j in range(qh):
                qs = slice(j * HEAD, (j + 1) * HEAD)
                ks = slice(j // group * HEAD, (j // group + 1) * HEAD)
                qj, kj, vj, g = q[:, qs], ky[:, ks], v[:, ks], ga[:, qs]
                e = jnp.where(ok, jnp.exp(mm_t(qj, kj) * scale), 0.0)
                inv = 1.0 / jnp.sum(e, -1, keepdims=True)
                eb = e.astype(BF)
                attn = mm(eb, vj) * inv
                gsc = (g * inv).astype(BF)
                dt = -jnp.sum(g * attn, -1, keepdims=True) * inv
                dv[j // group] += mt_m(eb, gsc)
                ds = (e * (mm_t(gsc, vj) + dt)).astype(BF)
                dk[j // group] += mt_m(ds, qj) * scale
                a = raw[:, qs]
                back, dg = norm_back(a, inv_rms(a), gqk_ref[0:1, :], rotate(mm(ds, kj) * scale, cs, -sn))
                draw[:, qs] = back.astype(BF)
                dgq += jnp.sum(dg, 0, keepdims=True)
            for j in range(kh):
                ks = slice(qc + j * HEAD, qc + (j + 1) * HEAD)
                a = raw[:, ks]
                back, dg = norm_back(a, inv_rms(a), gqk_ref[1:2, :], rotate(dk[j], cs, -sn))
                draw[:, ks] = back.astype(BF)
                dgk += jnp.sum(dg, 0, keepdims=True)
                draw[:, qc + kw + j * HEAD : qc + kw + (j + 1) * HEAD] = dv[j].astype(BF)
            gs_ref[...] = mt_m(h_ref[...], draw[...]).astype(BF)
            dh = mm_t(draw[...], w[...])
            split_whole(dh, own, send)
            total = jnp.zeros((1, width), F32)
            for b in range(2 * C):
                x = xb[b // C][b % C * half : (b % C + 1) * half, :].astype(F32)
                total += jnp.sum(dh[b * half : (b + 1) * half] * (x * inv_rms(x)), 0, keepdims=True)
            gn[0:1, :] = total
            gn[1:2, :] = dgf[...]
            ex[...] = jnp.zeros_like(ex)
            for a in range(F):
                for b in range(C):
                    dest = (mf ^ mask_of(a, F, mt)) * C + (mc ^ b)
                    gb[a // FH][a % FH, b * rows : (b + 1) * rows, :] = gs_ref[at(dest * rows, rows, rows), :]
                    blk = at(dest * rows // 128 * 128, 128, 128)
                    ex[2 * b : 2 * b + 1, 0:128] = gn[0:1, blk]
                    ex[2 * b : 2 * b + 1, 128:256] = gn[1:2, blk]
                    ex[2 * b : 2 * b + 1, 256:384] = dgq
                    ex[2 * b + 1 : 2 * b + 2, 0:128] = dgk
                gb[a // FH][a % FH, CR:, :] = ex[...].astype(BF)

        res = call(
            attn_back,
            whole + [shape(FH, CR + 2 * C, aw)] * 2,
            xs + [g_att, h, raw, q, ky, v, w_qkv, gv, gqk, cos, sin, allowed, dg_ffn],
            [pltpu.VMEM((R, aw), BF), pltpu.VMEM((width, aw), BF), pltpu.VMEM((2 * C, aw), F32), pltpu.VMEM((8, width), F32)],
            flops=4 * R * width * aw + 12 * R * R * qc,
        )
        gq = reduce_blocks(res[2], after(res[3], o_first[0]), "fsdp", F, gate=units_first[0]).astype(BF)
        gf = jnp.concatenate([g_units.astype(BF), g_down.astype(BF)], -1)
        gf = scatter([gf[0]] + [gf[k] for k in range(1, F)], "fsdp", F)

        def ffn_owner(*refs):
            b, outs = refs[:F], refs[F:]
            mf, _ = me()
            for k in range(F):
                d = at((mf ^ k) * hp, hp, 128)
                for m in range(3):
                    outs[m][:, d] = b[k][:, m * hp : (m + 1) * hp].astype(F32)

        ffn_grads = call(ffn_owner, [shape(rows, F * hp, dtype=F32)] * 3, gf)
        if hp > hc:
            ffn_grads = [g.reshape(rows, F, hp)[:, :, :hc].reshape(rows, F * hc) for g in ffn_grads]
        go = go.astype(BF)
        ga = []
        for j in range(C):
            both_grads = jnp.concatenate([gq[j * rows : (j + 1) * rows], go[j * rows : (j + 1) * rows]], 1)
            gains = jnp.pad(gq[CR + 2 * j : CR + 2 * j + 2], ((0, 6), (0, qc)))
            ga.append(jnp.concatenate([both_grads, gains], 0))
        ga = scatter([ga[0]] + list(after(ga[1:], g_units)), "context", C)
        dh = reduce(res[0], res[1], None, "context", C, enter=units_first[0])[0]
        x32 = x_half.astype(F32)
        inward, _ = norm_back(x32, inv_rms(x32), gv[0:1], dh)
        grad_hidden = (dx_mid + inward).astype(BF)

        def attn_owner(*refs):
            b, gwq, gwk, gwv, gwo, ge = refs[:C], *refs[C:]
            _, mc = me()
            if share > 1:
                gwk[...] = jnp.zeros_like(gwk)
                gwv[...] = jnp.zeros_like(gwv)
            e = jnp.zeros((8, aw), F32)
            for j in range(C):
                d = mc ^ j
                gwq[:, at(d * qc, qc, 128)] = b[j][0:rows, :qc].astype(F32)
                gwo[:, at(d * qc, qc, 128)] = b[j][0:rows, aw:].astype(F32)
                ks = at(d * kv_local // C * HEAD, kw, 128)
                gk = b[j][0:rows, qc : qc + kw].astype(F32)
                gw = b[j][0:rows, qc + kw : aw].astype(F32)
                if share > 1:
                    gwk[:, ks] += gk
                    gwv[:, ks] += gw
                else:
                    gwk[:, ks] = gk
                    gwv[:, ks] = gw
                e += b[j][rows:, :aw].astype(F32)
            ge[...] = e

        gwq, gwk, gwv, gwo, ge = call(
            attn_owner,
            [
                shape(rows, C * qc, dtype=F32), shape(rows, kv_local * HEAD, dtype=F32),
                shape(rows, kv_local * HEAD, dtype=F32), shape(rows, C * qc, dtype=F32), shape(8, aw, dtype=F32),
            ],
            ga,
        )
        ge = ge + swap_t(ge)

        def piece(row, start, off, size):
            return lax.dynamic_slice(ge, (row, start + off), (1, size)).reshape(size)

        return (
            both_halves(out).reshape(1, tokens, width),
            both_halves(grad_hidden).reshape(1, tokens, width),
            gwq, gwk, gwv, gwo.T,
            ffn_grads[0], ffn_grads[1], ffn_grads[2].T,
            piece(0, 0, lane, rows), piece(0, 128, lane, rows), piece(0, 256, goff, grow), piece(1, 0, goff, grow),
        )

    both = ("fsdp", "context")
    seq, row, col, vec = P("fsdp", "context", None), P(both, "tensor"), P("tensor", both), P(both)
    return jax.shard_map(
        local,
        mesh=mesh,
        in_specs=(seq, P("fsdp", "context"), row, row, row, col, row, row, col, vec, vec, vec, vec, seq),
        out_specs=(seq, seq, row, row, row, col, row, row, col, vec, vec, vec, vec),
        check_vma=False,
    )
```

```python
import jax
import jax.numpy as jnp
from jax import lax
from jax.experimental import pallas as pl
from jax.experimental.pallas import tpu as pltpu
from jax.sharding import PartitionSpec as P

HEAD = 128
EPS = 1e-06
THETA = 1000000.0
BF = jnp.bfloat16
F32 = jnp.float32


def mm(a, b):
    return lax.dot_general(a, b, (((1,), (0,)), ((), ())), preferred_element_type=F32)


def mm_t(a, b):
    return lax.dot_general(a, b, (((1,), (1,)), ((), ())), preferred_element_type=F32)


def mt_m(a, b):
    return lax.dot_general(a, b, (((0,), (0,)), ((), ())), preferred_element_type=F32)


def inv_rms(v):
    return lax.rsqrt(jnp.mean(v * v, axis=-1, keepdims=True) + EPS)


def norm_back(v, r, g, up):
    n = v * r
    w = up * g
    return r * (w - n * jnp.mean(w * n, axis=-1, keepdims=True)), up * n


def swap(x, axis, n, k):
    return lax.ppermute(x, axis, [(i, i ^ k) for i in range(n)])


def bits(n):
    return n.bit_length() - 1


def turned(j, n):
    return sum(((j >> i) & 1) << (bits(n) - 1 - i) for i in range(bits(n)))


def mask_of(j, n, t):
    return j + t * (turned(j, n) - j)


def hop(x, axis, n, i):
    steps = [1 << i, 1 << (bits(n) - 1 - i)]
    return lax.ppermute(x, (axis, "tensor"), [(2 * d + t, 2 * (d ^ steps[t]) + t) for d in range(n) for t in range(2)])


def scatter(blocks, axis, n):
    got = {k: swap(blocks[k], axis, n, k) for k in range(n - 1, 0, -1)}
    return [blocks[0]] + [got[k] for k in range(1, n)]


def join(a, b):
    def body(a_ref, b_ref, o_ref):
        o_ref[: a.shape[0]] = a_ref[...]
        o_ref[a.shape[0] :] = b_ref[...]

    return call(body, [shape(2 * a.shape[0], *a.shape[1:])], [a, b], vmem_mb=8)[0]


def gather(x, axis, n, gate=None, first=None):
    x = x[None]
    for i in range(bits(n)):
        got = hop(x, axis, n, i)
        if first is not None and i == 0:
            first.append(got)
        if i < bits(n) - 1:
            x = join(x, got if gate is None else after(got, gate))
    return [x, got]


def reduce_blocks(low, high, axis, n, gate=None, first=None, last=None):
    for i in range(bits(n) - 1, -1, -1):
        got = hop(high, axis, n, i)
        if first is not None and i == bits(n) - 1:
            first.append(got)
        if gate is not None and i:
            got = after(got, gate)
        if last is not None and not i:
            got = after(got, last)
        low = low.astype(F32) + got.astype(F32)
        if i:
            keep = low.shape[0] // 2
            low, high = low[:keep], low[keep:].astype(BF)
    return low[0]


def after(x, *deps):
    return lax.optimization_barrier((x, deps))[0]


def at(offset, size, unit):
    return pl.ds(pl.multiple_of(offset, unit), size)


def call(body, outs, args, scratch=(), flops=0, vmem_mb=20, hbm=0, hbm_outs=0):
    vmem = pl.BlockSpec(memory_space=pltpu.VMEM)
    far = pl.BlockSpec(memory_space=pltpu.MemorySpace.HBM)
    moved = sum(a.size * a.dtype.itemsize for a in list(args) + list(outs))
    return pl.pallas_call(
        body,
        out_shape=list(outs),
        in_specs=[far] * hbm + [vmem] * (len(args) - hbm),
        out_specs=[far] * hbm_outs + [vmem] * (len(outs) - hbm_outs),
        scratch_shapes=list(scratch),
        cost_estimate=pl.CostEstimate(flops=flops, bytes_accessed=moved, transcendentals=0),
        compiler_params=pltpu.CompilerParams(vmem_limit_bytes=vmem_mb * 1024 * 1024),
    )(*args)


def shape(*s, dtype=BF):
    return jax.ShapeDtypeStruct(s, dtype)


def solution(mesh):
    F, C, T = mesh.shape["fsdp"], mesh.shape["context"], mesh.shape["tensor"]

    def local(
        hidden, segments, w_query, w_key, w_value, w_out, w_gate, w_up, w_down,
        gain_attn, gain_ffn, gain_query, gain_key, cotangent,
    ):
        f, c, t = lax.axis_index("fsdp"), lax.axis_index("context"), lax.axis_index("tensor")
        tokens, width = hidden.shape[1], hidden.shape[2]
        half = tokens // T
        rows = w_query.shape[0]
        grow = gain_query.shape[0]
        kv_local = w_key.shape[1] // HEAD
        qc = w_query.shape[1] // C
        kw = max(HEAD, w_key.shape[1] // C)
        hc = w_gate.shape[1] // F
        hp = -(-hc // 128) * 128
        qh, kh = qc // HEAD, kw // HEAD
        group = qh // kh
        aw = qc + 2 * kw
        CR = C * rows
        R = T * C * half
        H = R // 2
        scale = HEAD ** (-0.5)
        share = kw * C // w_key.shape[1]
        wide = aw + qc + width
        CH, FH = C // 2, F // 2

        lane = (f * C + c) * rows % 128
        goff = (f * C + c) * grow

        hid = hidden.reshape(tokens, width)
        tall = max(rows, half)

        def me():
            return lax.axis_index("fsdp"), lax.axis_index("context")

        def ffn_pack(wg_ref, wu_ref, wd_ref, *refs):
            outs, sem = refs[:F], refs[F]
            mf, _ = me()
            copies = []
            for k in range(F):
                for j, w in enumerate((wg_ref, wu_ref, wd_ref)):
                    copies.append(pltpu.make_async_copy(w.at[:, at((mf ^ k) * hp, hp, 128)], outs[k].at[:, j * hp : (j + 1) * hp], sem.at[k, j]))
            for cp in copies:
                cp.start()
            for cp in copies:
                cp.wait()

        w_down = w_down.T
        if hp > hc:
            fill = [((0, 0), (0, 0), (0, hp - hc))]
            w_gate, w_up, w_down = [jnp.pad(w.reshape(rows, F, hc), *fill).reshape(rows, F * hp) for w in (w_gate, w_up, w_down)]
        def attn_pack(wq_ref, wk_ref, wv_ref, wo_ref, x_ref, ga_ref, gf_ref, gq_ref, gk_ref, s_ref, *refs):
            outs, sem = refs[:C], refs[C]
            mt = lax.axis_index("tensor")
            mf, mc = me()
            copies = []
            for k in range(C):
                d = mc ^ k
                ks = at(d * kv_local // C * HEAD, kw, 128)
                qs = at(d * qc, qc, 128)
                parts = [(wq_ref, qs, 0, qc), (wk_ref, ks, qc, kw), (wv_ref, ks, qc + kw, kw), (wo_ref, qs, aw, qc)]
                copies.append(pltpu.make_async_copy(x_ref.at[at(mt * half, half, half), :], outs[k].at[0:half, aw + qc :], sem.at[k, 4]))
                for m, (w, src, start, size) in enumerate(parts):
                    copies.append(pltpu.make_async_copy(w.at[:, src], outs[k].at[0:rows, start : start + size], sem.at[k, m]))
            for cp in copies:
                cp.start()
            dest = mf * C + mc
            lanes = lax.broadcasted_iota(jnp.int32, (8, 128), 1)
            docs = jnp.broadcast_to(s_ref[...].astype(F32), (8, 128))
            docs = jnp.where((lanes < half) == (mt == 0), docs, pltpu.roll(docs, half, 1))

            def placed(ref, want):
                size = ref.shape[1]
                r = lax.broadcasted_iota(jnp.int32, (size, 128), 0)
                pick = (lax.broadcasted_iota(jnp.int32, (size, 128), 1) == r + want).astype(F32).astype(BF)
                return mm(jnp.broadcast_to(ref[...].astype(F32), (8, size)).astype(BF), pick)[0:1]

            ln, hd = dest * rows % 128, dest * grow
            blank = jnp.zeros((1, aw - 384), F32) if aw > 384 else None
            first = [placed(ga_ref, ln), placed(gf_ref, ln), placed(gq_ref, hd)]
            first = jnp.concatenate(first + ([blank] if aw > 384 else []), 1)
            second = jnp.concatenate([placed(gk_ref, hd), jnp.zeros((1, aw - 128), F32)], 1)
            ext = jnp.concatenate([first, second, jnp.zeros((6, aw), F32)], 0).astype(BF)
            for k in range(C):
                outs[k][tall:, :aw] = ext
                outs[k][tall:, aw : aw + qc] = jnp.zeros((8, qc), BF)
                outs[k][tall:, aw + qc : aw + qc + 128] = docs.astype(BF)
                outs[k][tall:, aw + qc + 128 :] = jnp.zeros((8, width - 128), BF)
            for cp in copies:
                cp.wait()

        wa = call(
            attn_pack,
            [shape(tall + 8, wide)] * C,
            [w_query, w_key, w_value, w_out.T, hid]
            + [v.reshape(1, -1) for v in (gain_attn, gain_ffn, gain_query, gain_key)]
            + [segments.reshape(1, tokens)],
            [pltpu.SemaphoreType.DMA((C, 5))],
            hbm=5,
            vmem_mb=60,
        )

        wf = call(
            ffn_pack,
            [shape(rows, 3 * hp)] * F,
            list(after((w_gate, w_up, w_down), wa[0])),
            [pltpu.SemaphoreType.DMA((F, 3))],
            hbm=3,
            vmem_mb=60,
        )
        wa_got = scatter(wa, "context", C)

        wf = scatter(wf, "fsdp", F)

        def attn_join(*refs):
            b, qkv, o, x, docs = refs[:C], refs[C], refs[C + 1], refs[C + 2], refs[C + 3]
            mt = lax.axis_index("tensor")
            docs[...] = jnp.zeros_like(docs)
            for k in range(C):
                j = mask_of(k, C, mt)
                qkv[k * rows : (k + 1) * rows, :] = b[k][0:rows, :aw]
                o[k * rows : (k + 1) * rows, :] = b[k][0:rows, aw : aw + qc]
                x[at(j * half, half, half), :] = b[k][0:half, aw + qc :]
                docs[pl.ds(j, 1), :] = b[k][tall:, aw + qc : aw + qc + 128].astype(F32)[0:1]
            x[C * half :, :128] = docs[...].astype(BF)
            x[C * half :, 128:] = jnp.zeros((8, width - 128), BF)
            qkv[CR:, :] = jnp.concatenate([b[k][tall:, :aw].astype(F32)[0:2] for k in range(C)], 0).astype(BF)

        wq, wo, x_own = call(
            attn_join,
            [shape(CR + 2 * C, aw), shape(CR, qc), shape(C * half + 8, width)],
            [after(wa_got[0], wf[1])] + wa_got[1:],
            [pltpu.VMEM((8, 128), F32)],
        )
        def ffn_join(*refs):
            for k in range(F):
                refs[F][k] = refs[k][...]

        wf_got = wf
        wf = call(ffn_join, [shape(F, rows, 3 * hp)], [after(wf[0], wq)] + wf[1:], vmem_mb=8)[0]
        wf_first = hop(wf[None], "context", C, 0)
        wf_here = wf[None]

        q_here = []
        wq = gather(wq, "fsdp", F, gate=wf, first=q_here)
        wo = gather(after(wo, wq[0]), "fsdp", F)

        def my_half(x):
            return lax.dynamic_slice_in_dim(x, t * half, half, 0)

        def other_half(x):
            return lax.dynamic_slice_in_dim(x, (1 - t) * half, half, 0)

        def swap_t(x):
            return swap(x, "tensor", T, 1)

        x_half = my_half(hid)
        xs = [x_own, swap_t(x_own)]

        idx = jnp.arange(R, dtype=jnp.int32)
        trel, k, i = idx // (C * half), (idx // half) % C, idx % half
        pos = (c ^ mask_of(k, C, t ^ trel)) * tokens + (t ^ trel) * half + i
        freq = THETA ** (-(jnp.arange(HEAD // 2, dtype=F32) * 2.0 / HEAD))
        angle = pos.astype(F32)[:, None] * freq[None, :]
        cos, sin = jnp.cos(angle), jnp.sin(angle)
        cos, sin = jnp.concatenate([cos, cos], 1), jnp.concatenate([-sin, sin], 1)
        pos_row = jnp.broadcast_to(pos[None], (8, R))
        pos_col = jnp.broadcast_to(pos[:, None], (R, 128))

        def find_allowed(a_ref, b_ref, pr_ref, pc_ref, out):
            copies = CH * (2 * half // 128)
            row = []
            for ref in (a_ref, b_ref):
                d = ref[C * half :, :128].astype(F32)
                d = jnp.concatenate([d] * (C * half // 128), 1)
                keep = lax.broadcasted_iota(jnp.int32, d.shape, 1) // half == lax.broadcasted_iota(jnp.int32, d.shape, 0)
                row.append(jnp.sum(jnp.where(keep, d, 0.0), 0, keepdims=True))
            row = jnp.broadcast_to(jnp.concatenate(row, 1), (8, R))
            first = (lax.broadcasted_iota(jnp.int32, (8, 128), 0) == 0).astype(F32).astype(BF)
            col = mt_m(row.astype(BF), first)
            pc = pc_ref[...]
            for m in range(R // 128):
                sl = slice(m * 128, (m + 1) * 128)
                ok = (col == row[0:1, sl]) & (pc >= pr_ref[0:1, sl])
                out[:, sl] = jnp.where(ok, 1.0, 0.0).astype(BF)

        allowed = call(find_allowed, [shape(R, R)], xs + [pos_row, pos_col])[0]

        def reduce(own, low, high, axis, n, enter=None, first=None, last=None):
            keep = H // 2
            if high is None:
                low = swap_t(low)
                low, high = low[:keep], low[keep:]
            else:
                low, high = swap_t(low), swap_t(high)
            high = (own[keep:] + high.astype(F32)).astype(BF)
            low = own[:keep] + low.astype(F32)
            if enter is not None:
                high = after(high, enter)
            shaped = (n // 2, half, width)
            return reduce_blocks(low.reshape(shaped), high.reshape(shaped), axis, n, None, first, last), high

        def spread(x, axis, n):
            b = [x]
            for i in range(bits(n)):
                b = b + [hop(a, axis, n, i) for a in b]
            return b + [swap_t(a) for a in b]

        def both_halves(x):
            y = swap_t(x)
            return jnp.where(t == 0, jnp.concatenate([x, y], 0), jnp.concatenate([y, x], 0))

        cot = cotangent.reshape(tokens, width)
        def rotate(v, cs, sn):
            return v * cs + pltpu.roll(v, HEAD // 2, 1) * sn

        def split_rows(p, own, low, high):
            own[...] = p[:H]
            low[...] = p[H : H + H // 2].astype(BF)
            high[...] = p[H + H // 2 :].astype(BF)

        def split_whole(p, own, send):
            own[...] = p[:H]
            send[...] = p[H:].astype(BF)

        whole = [shape(H, width, dtype=F32), shape(H, width)]
        halves = [shape(H, width, dtype=F32), shape(H // 2, width), shape(H // 2, width)]

        got = after(wf_first, q_here[0])
        for i in range(1, bits(C)):
            wf_here = join(wf_here, got)
            got = hop(wf_here, "context", C, i)
        wf = [wf_here, got]

        def attn_fwd(*refs):
            xb, wb, refs = refs[:2], refs[2:4], refs[4:]
            cs_ref, sn_ref, ok_ref = refs[:3]
            outs, o, gv, gqk = refs[3:9], refs[9], refs[10], refs[11]
            h, raw, q, ky, v, w = refs[12:18]
            sem = refs[18]
            mf, mc = me()
            mt = lax.axis_index("tensor")
            sent = [pltpu.make_async_copy(a, b, sem.at[m]) for m, (a, b) in enumerate(zip((h, raw, q, ky, v, w), outs))]
            gv[...] = jnp.zeros_like(gv)
            acc = jnp.zeros((2, 128), F32)
            for a in range(F):
                wa_ref = wb[a // FH]
                e = wa_ref[a % FH, CR:, :].astype(F32)
                for b in range(C):
                    dest = (mf ^ mask_of(a, F, mt)) * C + (mc ^ b)
                    w[at(dest * rows, rows, rows), :] = wa_ref[a % FH, b * rows : (b + 1) * rows, :]
                    blk = at(dest * rows // 128 * 128, 128, 128)
                    gv[0:1, blk] += e[2 * b : 2 * b + 1, 0:128]
                    gv[1:2, blk] += e[2 * b : 2 * b + 1, 128:256]
                    acc += jnp.concatenate([e[2 * b : 2 * b + 1, 256:384], e[2 * b + 1 : 2 * b + 2, 0:128]], 0)
            gqk[0:2, :] = acc
            g = gv[0:1, :]
            for b in range(2 * C):
                x = xb[b // C][b % C * half : (b % C + 1) * half, :].astype(F32)
                h[b * half : (b + 1) * half, :] = (x * inv_rms(x) * g).astype(BF)
            sent[0].start()
            sent[5].start()
            p = mm(h[...], w[...])
            raw[...] = p[:, : qc + kw]
            v[...] = p[:, qc + kw :].astype(BF)
            sent[1].start()
            sent[4].start()
            cs, sn = cs_ref[...], sn_ref[...]
            for j in range(qh + kh):
                a = p[:, j * HEAD : (j + 1) * HEAD]
                gg = gqk[0:1, :] if j < qh else gqk[1:2, :]
                rot = rotate(a * inv_rms(a) * gg, cs, sn).astype(BF)
                if j < qh:
                    q[:, j * HEAD : (j + 1) * HEAD] = rot
                else:
                    ky[:, (j - qh) * HEAD : (j - qh + 1) * HEAD] = rot
            sent[2].start()
            sent[3].start()
            ok = ok_ref[...].astype(F32) > 0.5
            for j in range(qh):
                qs = slice(j * HEAD, (j + 1) * HEAD)
                ks = slice(j // group * HEAD, (j // group + 1) * HEAD)
                e = jnp.where(ok, jnp.exp(mm_t(q[:, qs], ky[:, ks]) * scale), 0.0)
                o[:, qs] = (mm(e.astype(BF), v[:, ks]) / jnp.sum(e, -1, keepdims=True)).astype(BF)
            for cp in sent:
                cp.wait()

        kept = [shape(R, width), shape(R, qc + kw, dtype=F32), shape(R, qc), shape(R, kw), shape(R, kw), shape(width, aw)]
        h, raw, q, ky, v, w_qkv, o, gv, gqk = call(
            attn_fwd,
            kept + [shape(R, qc), shape(8, width, dtype=F32), shape(8, 128, dtype=F32)],
            xs + wq + [cos, sin, after(allowed, wf_first, wo[0])],
            [pltpu.VMEM(a.shape, a.dtype) for a in kept] + [pltpu.SemaphoreType.DMA((6,))],
            flops=2 * R * width * aw + 4 * R * R * qc,
            hbm_outs=6,
        )

        dys = gather(after(my_half(cot), gv), "fsdp", F)
        dys = dys + [swap_t(b) for b in dys]

        def ffn_pre(*refs):
            wb, db, w, dy, du = refs[:2], refs[2:6], *refs[6:]
            mf, mc = me()
            mt = lax.axis_index("tensor")
            for a in range(C):
                for b in range(F):
                    dest = (mf ^ b) * C + (mc ^ mask_of(a, C, mt))
                    w[at(dest * rows, rows, rows), :] = wb[a // CH][a % CH, b]
            for b in range(2 * F):
                dy[b * half : (b + 1) * half, :] = db[b // FH][b % FH]
            du[...] = mm(dy[...], w[:, 2 * hp :])

        w_f, dy, du = call(
            ffn_pre,
            [shape(width, 3 * hp), shape(R, width), shape(R, hp, dtype=F32)],
            wf + dys,
            flops=2 * R * width * hp,
        )

        def out_proj(o_ref, *refs):
            wb, own, low, high, w = refs[:2], *refs[2:]
            mf, mc = me()
            mt = lax.axis_index("tensor")
            for a in range(F):
                for b in range(C):
                    dest = (mf ^ mask_of(a, F, mt)) * C + (mc ^ b)
                    w[at(dest * rows, rows, rows), :] = wb[a // FH][a % FH, b * rows : (b + 1) * rows, :]
            split_rows(mm_t(o_ref[...], w[...]), own, low, high)

        res = call(
            out_proj,
            halves + [shape(width, qc)],
            [after(o, wf[1])] + wo,
            flops=2 * R * width * qc,
        )
        w_o = res[3]
        x_mid = x_half.astype(F32) + reduce(*res[:3], "context", C, last=du)[0]
        r2 = inv_rms(x_mid)
        g_ffn = gv[1:2]
        h2s = spread((x_mid * r2 * g_ffn).astype(BF), "fsdp", F)

        def ffn_main(*refs):
            hb, w, du_ref, own, low, high, h2, act = refs[: 2 * F], *refs[2 * F :]
            for b in range(2 * F):
                h2[b * half : (b + 1) * half, :] = hb[b][...]
            p = mm(h2[...], w[:, : 2 * hp])
            gate, up = p[:, :hp], p[:, hp:]
            sg = 1.0 / (1.0 + jnp.exp(-gate))
            d = du_ref[...]
            sl = gate * sg
            act[:, :hp] = (d * up * sg * (1.0 + gate * (1.0 - sg))).astype(BF)
            act[:, hp : 2 * hp] = (d * sl).astype(BF)
            act[:, 2 * hp :] = (sl * up).astype(BF)
            split_rows(mm_t(act[:, : 2 * hp], w[:, : 2 * hp]), own, low, high)

        res = call(
            ffn_main,
            halves + [shape(R, width), shape(R, 3 * hp)],
            h2s + [w_f, du],
            flops=8 * R * width * hp,
        )
        h2, act = res[3:]
        dh2, dh2_sent = reduce(*res[:3], "fsdp", F)
        act = after(act, dh2_sent)

        def ffn_post(h2_ref, dy_ref, act_ref, w, *refs):
            own, send, gd, gu, g = refs[0], refs[1], refs[2:4], refs[4:6], refs[6]
            mf, mc = me()
            mt = lax.axis_index("tensor")
            g[:, : 2 * hp] = mt_m(h2_ref[...], act_ref[:, : 2 * hp]).astype(BF)
            g[:, 2 * hp :] = mt_m(dy_ref[...], act_ref[:, 2 * hp :]).astype(BF)
            for a in range(C):
                for b in range(F):
                    dest = (mf ^ b) * C + (mc ^ mask_of(a, C, mt))
                    src = at(dest * rows, rows, rows)
                    gu[a // CH][a % CH, b] = g[src, : 2 * hp]
                    gd[a // CH][a % CH, b] = g[src, 2 * hp :]
            split_whole(mm_t(act_ref[:, 2 * hp :], w[:, 2 * hp :]), own, send)

        res = call(
            ffn_post,
            whole + [shape(CH, F, rows, hp)] * 2 + [shape(CH, F, rows, 2 * hp)] * 2,
            [h2, dy, act, w_f],
            [pltpu.VMEM((width, 3 * hp), BF)],
            flops=8 * R * width * hp,
        )
        out_parts, down_parts, units_parts = list(res[:2]) + [None], res[2:4], res[4:6]

        inward, gn_rows = norm_back(x_mid, r2, g_ffn, dh2)
        dg_ffn = jnp.sum(gn_rows, 0, keepdims=True)
        dx_mid = my_half(cot).astype(F32) + inward
        dx_low = dx_mid.astype(BF)
        dxs = spread(dx_low, "context", C)
        units_first, out_first = [], []
        g_units = reduce_blocks(*after(units_parts, dxs[1:C]), "context", C, first=units_first)
        out = (x_mid + reduce(*out_parts, "fsdp", F, enter=dx_low, first=out_first)[0]).astype(BF)

        far = [after(w_o, out_first[0]), q, ky, v, raw, h, w_qkv]

        def attn_back(*refs):
            far, refs = refs[:7], refs[7:]
            xb, db, refs = refs[:2], refs[2 : 2 + 2 * C], refs[2 + 2 * C :]
            gv_ref, gqk_ref, cs_ref, sn_ref, ok_ref, dgf, own, send = refs[:8]
            gb, dx, draw, gs_ref, ex, gn, ga = refs[8:10], *refs[10:16]
            wo_ref, q, ky, v, raw, h_ref, w = refs[16:23]
            sem = refs[23]
            loads = [pltpu.make_async_copy(a, b, sem.at[m]) for m, (a, b) in enumerate(zip(far, refs[16:23]))]
            for cp in loads:
                cp.start()
            for b in range(2 * C):
                dx[b * half : (b + 1) * half, :] = db[b][...]
            loads[0].wait()
            ga[...] = mm(dx[...], wo_ref[...])
            for cp in loads[1:5]:
                cp.wait()
            mf, mc = me()
            mt = lax.axis_index("tensor")
            cs, sn = cs_ref[...], sn_ref[...]
            ok = ok_ref[...].astype(F32) > 0.5
            dk, dv = [0.0] * kh, [0.0] * kh
            dgq, dgk = jnp.zeros((1, HEAD), F32), jnp.zeros((1, HEAD), F32)
            for j in range(qh):
                qs = slice(j * HEAD, (j + 1) * HEAD)
                ks = slice(j // group * HEAD, (j // group + 1) * HEAD)
                qj, kj, vj, g = q[:, qs], ky[:, ks], v[:, ks], ga[:, qs]
                e = jnp.where(ok, jnp.exp(mm_t(qj, kj) * scale), 0.0)
                inv = 1.0 / jnp.sum(e, -1, keepdims=True)
                eb = e.astype(BF)
                attn = mm(eb, vj) * inv
                gsc = (g * inv).astype(BF)
                dt = -jnp.sum(g * attn, -1, keepdims=True) * inv
                dv[j // group] += mt_m(eb, gsc)
                ds = (e * (mm_t(gsc, vj) + dt)).astype(BF)
                dk[j // group] += mt_m(ds, qj) * scale
                a = raw[:, qs]
                back, dg = norm_back(a, inv_rms(a), gqk_ref[0:1, :], rotate(mm(ds, kj) * scale, cs, -sn))
                draw[:, qs] = back.astype(BF)
                dgq += jnp.sum(dg, 0, keepdims=True)
            for j in range(kh):
                ks = slice(qc + j * HEAD, qc + (j + 1) * HEAD)
                a = raw[:, ks]
                back, dg = norm_back(a, inv_rms(a), gqk_ref[1:2, :], rotate(dk[j], cs, -sn))
                draw[:, ks] = back.astype(BF)
                dgk += jnp.sum(dg, 0, keepdims=True)
                draw[:, qc + kw + j * HEAD : qc + kw + (j + 1) * HEAD] = dv[j].astype(BF)
            for cp in loads[5:]:
                cp.wait()
            gs_ref[...] = mt_m(h_ref[...], draw[...]).astype(BF)
            dh = mm_t(draw[...], w[...])
            split_whole(dh, own, send)
            total = jnp.zeros((1, width), F32)
            for b in range(2 * C):
                x = xb[b // C][b % C * half : (b % C + 1) * half, :].astype(F32)
                total += jnp.sum(dh[b * half : (b + 1) * half] * (x * inv_rms(x)), 0, keepdims=True)
            gn[0:1, :] = total
            gn[1:2, :] = dgf[...]
            ex[...] = jnp.zeros_like(ex)
            for a in range(F):
                for b in range(C):
                    dest = (mf ^ mask_of(a, F, mt)) * C + (mc ^ b)
                    gb[a // FH][a % FH, b * rows : (b + 1) * rows, :] = gs_ref[at(dest * rows, rows, rows), :]
                    blk = at(dest * rows // 128 * 128, 128, 128)
                    ex[2 * b : 2 * b + 1, 0:128] = gn[0:1, blk]
                    ex[2 * b : 2 * b + 1, 128:256] = gn[1:2, blk]
                    ex[2 * b : 2 * b + 1, 256:384] = dgq
                    ex[2 * b + 1 : 2 * b + 2, 0:128] = dgk
                gb[a // FH][a % FH, CR:, :] = ex[...].astype(BF)

        res = call(
            attn_back,
            whole + [shape(FH, CR + 2 * C, aw)] * 2 + [shape(R, width)],
            far + xs + dxs + [gv, gqk, cos, sin, allowed, dg_ffn],
            [pltpu.VMEM((R, aw), BF), pltpu.VMEM((width, aw), BF), pltpu.VMEM((2 * C, aw), F32), pltpu.VMEM((8, width), F32), pltpu.VMEM((R, qc), F32)]
            + [pltpu.VMEM(a.shape, a.dtype) for a in far]
            + [pltpu.SemaphoreType.DMA((7,))],
            hbm=7,
            flops=2 * R * width * qc + 4 * R * width * aw + 12 * R * R * qc,
            vmem_mb=24,
        )
        g_down = reduce_blocks(*down_parts, "context", C, gate=res[0])
        def out_grad(dx, o_ref, ga, gb, g):
            refs = (ga, gb)
            mf, mc = me()
            mt = lax.axis_index("tensor")
            g[...] = mt_m(dx[...], o_ref[...]).astype(BF)
            for a in range(F):
                for b in range(C):
                    dest = (mf ^ mask_of(a, F, mt)) * C + (mc ^ b)
                    refs[a // FH][a % FH, b * rows : (b + 1) * rows, :] = g[at(dest * rows, rows, rows), :]

        go = call(
            out_grad,
            [shape(FH, CR, qc)] * 2,
            [after(res[4], units_first[0]), o],
            [pltpu.VMEM((width, qc), BF)],
            flops=2 * R * width * qc,
        )
        dh, dh_sent = reduce(res[0], res[1], None, "context", C, enter=units_first[0])
        q_first = []
        gq = reduce_blocks(res[2], res[3], "fsdp", F, gate=(g_units, g_down, go[1], dh_sent), first=q_first).astype(BF)
        o_first = []
        go = reduce_blocks(go[0], go[1], "fsdp", F, first=o_first)
        gf = jnp.concatenate([g_units.astype(BF), g_down.astype(BF)], -1)
        gf = scatter([gf[0]] + list(after([gf[k] for k in range(1, F)], q_first[0], o_first[0])), "fsdp", F)

        def ffn_owner(*refs):
            b, outs = refs[:F], refs[F:]
            mf, _ = me()
            for k in range(F):
                d = at((mf ^ k) * hp, hp, 128)
                for m in range(3):
                    outs[m][:, d] = b[k][:, m * hp : (m + 1) * hp].astype(F32)

        ffn_grads = call(ffn_owner, [shape(rows, F * hp, dtype=F32)] * 3, gf)
        if hp > hc:
            ffn_grads = [g.reshape(rows, F, hp)[:, :, :hc].reshape(rows, F * hc) for g in ffn_grads]
        go = go.astype(BF)
        ga = []
        for j in range(C):
            both_grads = jnp.concatenate([gq[j * rows : (j + 1) * rows], go[j * rows : (j + 1) * rows]], 1)
            gains = jnp.pad(gq[CR + 2 * j : CR + 2 * j + 2], ((0, 6), (0, qc)))
            ga.append(jnp.concatenate([both_grads, gains], 0))
        ga = scatter(ga, "context", C)
        x32 = x_half.astype(F32)
        inward, _ = norm_back(x32, inv_rms(x32), gv[0:1], dh)
        grad_hidden = (dx_mid + inward).astype(BF)

        rows_out = [both_halves(out).reshape(1, tokens, width), both_halves(grad_hidden).reshape(1, tokens, width)]

        def attn_owner(*refs):
            b, gwq, gwk, gwv, gwo, ge = refs[:C], *refs[C:]
            _, mc = me()
            if share > 1:
                gwk[...] = jnp.zeros_like(gwk)
                gwv[...] = jnp.zeros_like(gwv)
            e = jnp.zeros((8, aw), F32)
            for j in range(C):
                d = mc ^ j
                gwq[:, at(d * qc, qc, 128)] = b[j][0:rows, :qc].astype(F32)
                gwo[:, at(d * qc, qc, 128)] = b[j][0:rows, aw:].astype(F32)
                ks = at(d * kv_local // C * HEAD, kw, 128)
                gk = b[j][0:rows, qc : qc + kw].astype(F32)
                gw = b[j][0:rows, qc + kw : aw].astype(F32)
                if share > 1:
                    gwk[:, ks] += gk
                    gwv[:, ks] += gw
                else:
                    gwk[:, ks] = gk
                    gwv[:, ks] = gw
                e += b[j][rows:, :aw].astype(F32)
            ge[...] = e

        gwq, gwk, gwv, gwo, ge = call(
            attn_owner,
            [
                shape(rows, C * qc, dtype=F32), shape(rows, kv_local * HEAD, dtype=F32),
                shape(rows, kv_local * HEAD, dtype=F32), shape(rows, C * qc, dtype=F32), shape(8, aw, dtype=F32),
            ],
            [after(ga[0], rows_out)] + ga[1:],
        )
        ge = ge + swap_t(ge)

        def piece(row, start, off, size):
            return lax.dynamic_slice(ge, (row, start + off), (1, size)).reshape(size)

        return (
            *rows_out,
            gwq, gwk, gwv, gwo.T,
            ffn_grads[0], ffn_grads[1], ffn_grads[2].T,
            piece(0, 0, lane, rows), piece(0, 128, lane, rows), piece(0, 256, goff, grow), piece(1, 0, goff, grow),
        )

    both = ("fsdp", "context")
    seq, row, col, vec = P("fsdp", "context", None), P(both, "tensor"), P("tensor", both), P(both)
    return jax.shard_map(
        local,
        mesh=mesh,
        in_specs=(seq, P("fsdp", "context"), row, row, row, col, row, row, col, vec, vec, vec, vec, seq),
        out_specs=(seq, seq, row, row, row, col, row, row, col, vec, vec, vec, vec),
        check_vma=False,
    )
```

```python
import jax
import jax.numpy as jnp
from jax import lax
from jax.experimental import pallas as pl
from jax.experimental.pallas import tpu as pltpu
from jax.sharding import PartitionSpec as P

HEAD = 128
EPS = 1e-06
THETA = 1000000.0
BF = jnp.bfloat16
F32 = jnp.float32


def mm(a, b):
    return lax.dot_general(a, b, (((1,), (0,)), ((), ())), preferred_element_type=F32)


def mm_t(a, b):
    return lax.dot_general(a, b, (((1,), (1,)), ((), ())), preferred_element_type=F32)


def mt_m(a, b):
    return lax.dot_general(a, b, (((0,), (0,)), ((), ())), preferred_element_type=F32)


def inv_rms(v):
    return lax.rsqrt(jnp.mean(v * v, axis=-1, keepdims=True) + EPS)


def norm_back(v, r, g, up):
    n = v * r
    w = up * g
    return r * (w - n * jnp.mean(w * n, axis=-1, keepdims=True)), up * n


def swap(x, axis, n, k):
    return lax.ppermute(x, axis, [(i, i ^ k) for i in range(n)])


def bits(n):
    return n.bit_length() - 1


def turned(j, n):
    return sum(((j >> i) & 1) << (bits(n) - 1 - i) for i in range(bits(n)))


def mask_of(j, n, t):
    return j + t * (turned(j, n) - j)


def hop(x, axis, n, i):
    steps = [1 << i, 1 << (bits(n) - 1 - i)]
    return lax.ppermute(x, (axis, "tensor"), [(2 * d + t, 2 * (d ^ steps[t]) + t) for d in range(n) for t in range(2)])


def scatter(blocks, axis, n):
    got = {k: swap(blocks[k], axis, n, k) for k in range(n - 1, 0, -1)}
    return [blocks[0]] + [got[k] for k in range(1, n)]


def join(a, b):
    def body(a_ref, b_ref, o_ref):
        o_ref[: a.shape[0]] = a_ref[...]
        o_ref[a.shape[0] :] = b_ref[...]

    return call(body, [shape(2 * a.shape[0], *a.shape[1:])], [a, b], vmem_mb=8)[0]


def gather(x, axis, n, gate=None, first=None):
    x = x[None]
    for i in range(bits(n)):
        got = hop(x, axis, n, i)
        if first is not None and i == 0:
            first.append(got)
        if i < bits(n) - 1:
            x = join(x, got if gate is None else after(got, gate))
    return [x, got]


def reduce_blocks(low, high, axis, n, gate=None, first=None, last=None):
    for i in range(bits(n) - 1, -1, -1):
        got = hop(high, axis, n, i)
        if first is not None and i == bits(n) - 1:
            first.append(got)
        if gate is not None and i:
            got = after(got, gate)
        if last is not None and not i:
            got = after(got, last)
        low = low.astype(F32) + got.astype(F32)
        if i:
            keep = low.shape[0] // 2
            low, high = low[:keep], low[keep:].astype(BF)
    return low[0]


def after(x, *deps):
    return lax.optimization_barrier((x, deps))[0]


def at(offset, size, unit):
    return pl.ds(pl.multiple_of(offset, unit), size)


def call(body, outs, args, scratch=(), flops=0, vmem_mb=20, hbm=0, hbm_outs=0):
    vmem = pl.BlockSpec(memory_space=pltpu.VMEM)
    far = pl.BlockSpec(memory_space=pltpu.MemorySpace.HBM)
    moved = sum(a.size * a.dtype.itemsize for a in list(args) + list(outs))
    outs = [pltpu.HBM(a.shape, a.dtype) for a in outs[:hbm_outs]] + list(outs[hbm_outs:])
    args = [pltpu.with_memory_space_constraint(a, pltpu.HBM) for a in args[:hbm]] + list(args[hbm:])
    return pl.pallas_call(
        body,
        out_shape=list(outs),
        in_specs=[far] * hbm + [vmem] * (len(args) - hbm),
        out_specs=[far] * hbm_outs + [vmem] * (len(outs) - hbm_outs),
        scratch_shapes=list(scratch),
        cost_estimate=pl.CostEstimate(flops=flops, bytes_accessed=moved, transcendentals=0),
        compiler_params=pltpu.CompilerParams(vmem_limit_bytes=vmem_mb * 1024 * 1024),
    )(*args)


def shape(*s, dtype=BF):
    return jax.ShapeDtypeStruct(s, dtype)


def solution(mesh):
    F, C, T = mesh.shape["fsdp"], mesh.shape["context"], mesh.shape["tensor"]

    def local(
        hidden, segments, w_query, w_key, w_value, w_out, w_gate, w_up, w_down,
        gain_attn, gain_ffn, gain_query, gain_key, cotangent,
    ):
        f, c, t = lax.axis_index("fsdp"), lax.axis_index("context"), lax.axis_index("tensor")
        tokens, width = hidden.shape[1], hidden.shape[2]
        half = tokens // T
        rows = w_query.shape[0]
        grow = gain_query.shape[0]
        kv_local = w_key.shape[1] // HEAD
        qc = w_query.shape[1] // C
        kw = max(HEAD, w_key.shape[1] // C)
        hc = w_gate.shape[1] // F
        hp = -(-hc // 128) * 128
        qh, kh = qc // HEAD, kw // HEAD
        group = qh // kh
        aw = qc + 2 * kw
        CR = C * rows
        R = T * C * half
        H = R // 2
        scale = HEAD ** (-0.5)
        share = kw * C // w_key.shape[1]
        wide = aw + qc + width
        CH, FH = C // 2, F // 2

        lane = (f * C + c) * rows % 128
        goff = (f * C + c) * grow

        hid = hidden.reshape(tokens, width)
        tall = max(rows, half)

        def me():
            return lax.axis_index("fsdp"), lax.axis_index("context")

        def ffn_pack(wg_ref, wu_ref, wd_ref, *refs):
            outs, sem = refs[:F], refs[F]
            mf, _ = me()
            copies = []
            for k in range(F):
                for j, w in enumerate((wg_ref, wu_ref, wd_ref)):
                    copies.append(pltpu.make_async_copy(w.at[:, at((mf ^ k) * hp, hp, 128)], outs[k].at[:, j * hp : (j + 1) * hp], sem.at[k, j]))
            for cp in copies:
                cp.start()
            for cp in copies:
                cp.wait()

        w_down = w_down.T
        if hp > hc:
            fill = [((0, 0), (0, 0), (0, hp - hc))]
            w_gate, w_up, w_down = [jnp.pad(w.reshape(rows, F, hc), *fill).reshape(rows, F * hp) for w in (w_gate, w_up, w_down)]
        def attn_pack(wq_ref, wk_ref, wv_ref, wo_ref, x_ref, ga_ref, gf_ref, gq_ref, gk_ref, s_ref, *refs):
            outs, sem, small = refs[:C], refs[C], refs[C + 1 : C + 6]
            mt = lax.axis_index("tensor")
            mf, mc = me()
            given = (ga_ref, gf_ref, gq_ref, gk_ref, s_ref)
            early = [pltpu.make_async_copy(a, b, sem.at[0, 5 + m]) for m, (a, b) in enumerate(zip(given, small))]
            for cp in early:
                cp.start()
            ga_ref, gf_ref, gq_ref, gk_ref, s_ref = small
            copies = []
            for k in range(C):
                d = mc ^ k
                ks = at(d * kv_local // C * HEAD, kw, 128)
                qs = at(d * qc, qc, 128)
                parts = [(wq_ref, qs, 0, qc), (wk_ref, ks, qc, kw), (wv_ref, ks, qc + kw, kw), (wo_ref, qs, aw, qc)]
                copies.append(pltpu.make_async_copy(x_ref.at[at(mt * half, half, half), :], outs[k].at[0:half, aw + qc :], sem.at[k, 4]))
                for m, (w, src, start, size) in enumerate(parts):
                    copies.append(pltpu.make_async_copy(w.at[:, src], outs[k].at[0:rows, start : start + size], sem.at[k, m]))
            for cp in copies:
                cp.start()
            for cp in early:
                cp.wait()
            dest = mf * C + mc
            lanes = lax.broadcasted_iota(jnp.int32, (8, 128), 1)
            docs = jnp.broadcast_to(s_ref[...].astype(F32), (8, 128))
            docs = jnp.where((lanes < half) == (mt == 0), docs, pltpu.roll(docs, half, 1))

            def placed(ref, want):
                size = ref.shape[1]
                r = lax.broadcasted_iota(jnp.int32, (size, 128), 0)
                pick = (lax.broadcasted_iota(jnp.int32, (size, 128), 1) == r + want).astype(F32).astype(BF)
                return mm(jnp.broadcast_to(ref[...].astype(F32), (8, size)).astype(BF), pick)[0:1]

            ln, hd = dest * rows % 128, dest * grow
            blank = jnp.zeros((1, aw - 384), F32) if aw > 384 else None
            first = [placed(ga_ref, ln), placed(gf_ref, ln), placed(gq_ref, hd)]
            first = jnp.concatenate(first + ([blank] if aw > 384 else []), 1)
            second = jnp.concatenate([placed(gk_ref, hd), jnp.zeros((1, aw - 128), F32)], 1)
            ext = jnp.concatenate([first, second, jnp.zeros((6, aw), F32)], 0).astype(BF)
            for k in range(C):
                outs[k][tall:, :aw] = ext
                outs[k][tall:, aw : aw + qc] = jnp.zeros((8, qc), BF)
                outs[k][tall:, aw + qc : aw + qc + 128] = docs.astype(BF)
                outs[k][tall:, aw + qc + 128 :] = jnp.zeros((8, width - 128), BF)
            for cp in copies:
                cp.wait()

        wa = call(
            attn_pack,
            [shape(tall + 8, wide)] * C,
            [w_query, w_key, w_value, w_out.T, hid]
            + [v.reshape(1, -1) for v in (gain_attn, gain_ffn, gain_query, gain_key)]
            + [segments.reshape(1, tokens)],
            [pltpu.SemaphoreType.DMA((C, 10))]
            + [pltpu.VMEM((1, v.shape[0]), BF) for v in (gain_attn, gain_ffn, gain_query, gain_key)]
            + [pltpu.VMEM((1, tokens), jnp.int32)],
            hbm=10,
            vmem_mb=16,
        )

        wf = call(
            ffn_pack,
            [shape(rows, 3 * hp)] * F,
            list(after((w_gate, w_up, w_down), wa[0])),
            [pltpu.SemaphoreType.DMA((F, 3))],
            hbm=3,
            vmem_mb=16,
        )
        wa_got = scatter(wa, "context", C)

        wf = scatter(wf, "fsdp", F)

        def attn_join(*refs):
            b, qkv, o, x, docs = refs[:C], refs[C], refs[C + 1], refs[C + 2], refs[C + 3]
            mt = lax.axis_index("tensor")
            docs[...] = jnp.zeros_like(docs)
            for k in range(C):
                j = mask_of(k, C, mt)
                qkv[k * rows : (k + 1) * rows, :] = b[k][0:rows, :aw]
                o[k * rows : (k + 1) * rows, :] = b[k][0:rows, aw : aw + qc]
                x[at(j * half, half, half), :] = b[k][0:half, aw + qc :]
                docs[pl.ds(j, 1), :] = b[k][tall:, aw + qc : aw + qc + 128].astype(F32)[0:1]
            x[C * half :, :128] = docs[...].astype(BF)
            x[C * half :, 128:] = jnp.zeros((8, width - 128), BF)
            qkv[CR:, :] = jnp.concatenate([b[k][tall:, :aw].astype(F32)[0:2] for k in range(C)], 0).astype(BF)

        wq, wo, x_own = call(
            attn_join,
            [shape(CR + 2 * C, aw), shape(CR, qc), shape(C * half + 8, width)],
            [after(wa_got[0], wf[1], wf[F - 1])] + wa_got[1:],
            [pltpu.VMEM((8, 128), F32)],
        )
        q_here = []
        wq = gather(wq, "fsdp", F, first=q_here)
        wo = gather(after(wo, wq[0]), "fsdp", F)

        def ffn_join(*refs):
            for k in range(F):
                refs[F][k] = refs[k][...]

        wf_got = wf
        wf = call(ffn_join, [shape(F, rows, 3 * hp)], [after(wf[0], q_here[0])] + wf[1:], vmem_mb=8)[0]
        wf_first = hop(wf[None], "context", C, 0)
        wf_here = wf[None]

        def my_half(x):
            return lax.dynamic_slice_in_dim(x, t * half, half, 0)

        def other_half(x):
            return lax.dynamic_slice_in_dim(x, (1 - t) * half, half, 0)

        def swap_t(x):
            return swap(x, "tensor", T, 1)

        x_half = my_half(hid)
        xs = [x_own, swap_t(x_own)]

        idx = jnp.arange(R, dtype=jnp.int32)
        trel, k, i = idx // (C * half), (idx // half) % C, idx % half
        pos = (c ^ mask_of(k, C, t ^ trel)) * tokens + (t ^ trel) * half + i
        freq = THETA ** (-(jnp.arange(HEAD // 2, dtype=F32) * 2.0 / HEAD))
        angle = pos.astype(F32)[:, None] * freq[None, :]
        cos, sin = jnp.cos(angle), jnp.sin(angle)
        cos, sin = jnp.concatenate([cos, cos], 1), jnp.concatenate([-sin, sin], 1)
        pos_row = jnp.broadcast_to(pos[None], (8, R))
        pos_col = jnp.broadcast_to(pos[:, None], (R, 128))

        def find_allowed(a_ref, b_ref, pr_ref, pc_ref, out):
            copies = CH * (2 * half // 128)
            row = []
            for ref in (a_ref, b_ref):
                d = ref[C * half :, :128].astype(F32)
                d = jnp.concatenate([d] * (C * half // 128), 1)
                keep = lax.broadcasted_iota(jnp.int32, d.shape, 1) // half == lax.broadcasted_iota(jnp.int32, d.shape, 0)
                row.append(jnp.sum(jnp.where(keep, d, 0.0), 0, keepdims=True))
            row = jnp.broadcast_to(jnp.concatenate(row, 1), (8, R))
            first = (lax.broadcasted_iota(jnp.int32, (8, 128), 0) == 0).astype(F32).astype(BF)
            col = mt_m(row.astype(BF), first)
            pc = pc_ref[...]
            for m in range(R // 128):
                sl = slice(m * 128, (m + 1) * 128)
                ok = (col == row[0:1, sl]) & (pc >= pr_ref[0:1, sl])
                out[:, sl] = jnp.where(ok, 1.0, 0.0).astype(BF)

        allowed = call(find_allowed, [shape(R, R)], xs + [pos_row, pos_col])[0]

        def pair_sum(own, low, high, enter=None):
            keep = H // 2
            if high is None:
                low = swap_t(low)
                low, high = low[:keep], low[keep:]
            else:
                low, high = swap_t(low), swap_t(high)
            high = (own[keep:] + high.astype(F32)).astype(BF)
            low = own[:keep] + low.astype(F32)
            if enter is not None:
                high = after(high, enter)
            return low, high

        def finish(low, high, axis, n, first=None, last=None):
            shaped = (n // 2, half, width)
            return reduce_blocks(low.reshape(shaped), high.reshape(shaped), axis, n, None, first, last)

        def reduce(own, low, high, axis, n, enter=None, first=None, last=None):
            low, high = pair_sum(own, low, high, enter)
            return finish(low, high, axis, n, first, last), high

        def spread(b, axis, n, start=0, late=None):
            for i in range(start, bits(n)):
                b = b + [hop(a, axis, n, i) for a in b]
            last = b[-1] if late is None else after(b[-1], late)
            return b + [swap_t(a) for a in b[:-1] + [last]]

        def both_halves(x):
            y = swap_t(x)
            return jnp.where(t == 0, jnp.concatenate([x, y], 0), jnp.concatenate([y, x], 0))

        cot = cotangent.reshape(tokens, width)
        def rotate(v, cs, sn):
            return v * cs + pltpu.roll(v, HEAD // 2, 1) * sn

        def split_rows(p, own, low, high):
            own[...] = p[:H]
            low[...] = p[H : H + H // 2].astype(BF)
            high[...] = p[H + H // 2 :].astype(BF)

        def split_whole(p, own, send):
            own[...] = p[:H]
            send[...] = p[H:].astype(BF)

        whole = [shape(H, width, dtype=F32), shape(H, width)]
        halves = [shape(H, width, dtype=F32), shape(H // 2, width), shape(H // 2, width)]

        got = after(wf_first, wo[0])
        for i in range(1, bits(C)):
            wf_here = join(wf_here, got)
            got = hop(wf_here, "context", C, i)
        wf = [wf_here, got]

        def attn_fwd(*refs):
            xb, wb, refs = refs[:2], refs[2:4], refs[4:]
            cs_ref, sn_ref, ok_ref = refs[:3]
            outs, o, gv, gqk = refs[3:9], refs[9], refs[10], refs[11]
            h, raw, q, ky, v, w = refs[12:18]
            sem = refs[18]
            mf, mc = me()
            mt = lax.axis_index("tensor")
            sent = [pltpu.make_async_copy(a, b, sem.at[m]) for m, (a, b) in enumerate(zip((h, raw, q, ky, v, w), outs))]
            gv[...] = jnp.zeros_like(gv)
            acc = jnp.zeros((2, 128), F32)
            for a in range(F):
                wa_ref = wb[a // FH]
                e = wa_ref[a % FH, CR:, :].astype(F32)
                for b in range(C):
                    dest = (mf ^ mask_of(a, F, mt)) * C + (mc ^ b)
                    w[at(dest * rows, rows, rows), :] = wa_ref[a % FH, b * rows : (b + 1) * rows, :]
                    blk = at(dest * rows // 128 * 128, 128, 128)
                    gv[0:1, blk] += e[2 * b : 2 * b + 1, 0:128]
                    gv[1:2, blk] += e[2 * b : 2 * b + 1, 128:256]
                    acc += jnp.concatenate([e[2 * b : 2 * b + 1, 256:384], e[2 * b + 1 : 2 * b + 2, 0:128]], 0)
            gqk[0:2, :] = acc
            g = gv[0:1, :]
            for b in range(2 * C):
                x = xb[b // C][b % C * half : (b % C + 1) * half, :].astype(F32)
                h[b * half : (b + 1) * half, :] = (x * inv_rms(x) * g).astype(BF)
            sent[0].start()
            sent[5].start()
            p = mm(h[...], w[...])
            raw[...] = p[:, : qc + kw]
            v[...] = p[:, qc + kw :].astype(BF)
            sent[1].start()
            sent[4].start()
            cs, sn = cs_ref[...], sn_ref[...]
            for j in range(qh + kh):
                a = p[:, j * HEAD : (j + 1) * HEAD]
                gg = gqk[0:1, :] if j < qh else gqk[1:2, :]
                rot = rotate(a * inv_rms(a) * gg, cs, sn).astype(BF)
                if j < qh:
                    q[:, j * HEAD : (j + 1) * HEAD] = rot
                else:
                    ky[:, (j - qh) * HEAD : (j - qh + 1) * HEAD] = rot
            sent[2].start()
            sent[3].start()
            ok = ok_ref[...].astype(F32) > 0.5
            for j in range(qh):
                qs = slice(j * HEAD, (j + 1) * HEAD)
                ks = slice(j // group * HEAD, (j // group + 1) * HEAD)
                e = jnp.where(ok, jnp.exp(mm_t(q[:, qs], ky[:, ks]) * scale), 0.0)
                o[:, qs] = (mm(e.astype(BF), v[:, ks]) / jnp.sum(e, -1, keepdims=True)).astype(BF)
            for cp in sent:
                cp.wait()

        kept = [shape(R, width), shape(R, qc + kw, dtype=F32), shape(R, qc), shape(R, kw), shape(R, kw), shape(width, aw)]
        h, raw, q, ky, v, w_qkv, o, gv, gqk = call(
            attn_fwd,
            kept + [shape(R, qc), shape(8, width, dtype=F32), shape(8, 128, dtype=F32)],
            xs + wq + [cos, sin, after(allowed, wf_first, wo[0])],
            [pltpu.VMEM(a.shape, a.dtype) for a in kept] + [pltpu.SemaphoreType.DMA((6,))],
            flops=2 * R * width * aw + 4 * R * R * qc,
            hbm_outs=6,
        )

        def out_proj(o_ref, *refs):
            wb, w_far, o_far, own, low, high, w, sem = refs[:2], *refs[2:]
            mf, mc = me()
            mt = lax.axis_index("tensor")
            kept = [pltpu.make_async_copy(o_ref, o_far, sem.at[0]), pltpu.make_async_copy(w, w_far, sem.at[1])]
            kept[0].start()
            for a in range(F):
                for b in range(C):
                    dest = (mf ^ mask_of(a, F, mt)) * C + (mc ^ b)
                    w[at(dest * rows, rows, rows), :] = wb[a // FH][a % FH, b * rows : (b + 1) * rows, :]
            kept[1].start()
            split_rows(mm_t(o_ref[...], w[...]), own, low, high)
            for cp in kept:
                cp.wait()

        res = call(
            out_proj,
            [shape(width, qc), shape(R, qc)] + halves,
            [o] + wo,
            [pltpu.VMEM((width, qc), BF), pltpu.SemaphoreType.DMA((2,))],
            hbm_outs=2,
            flops=2 * R * width * qc,
        )
        w_o, o = res[:2]
        low, high = pair_sum(*res[2:])
        branch_first = []
        x_mid = x_half.astype(F32) + finish(low, high, "context", C, first=branch_first)
        dys = gather(after(my_half(cot), gv), "fsdp", F, gate=branch_first[0])
        r2 = inv_rms(x_mid)
        g_ffn = gv[1:2]
        h2s = [(x_mid * r2 * g_ffn).astype(BF)]
        h2s = h2s + [hop(h2s[0], "fsdp", F, 0)]
        dys = dys + [swap_t(dys[0]), swap_t(after(dys[1], h2s[1]))]

        def ffn_pre(*refs):
            wb, db, w, dy, du = refs[:2], refs[2:6], *refs[6:]
            mf, mc = me()
            mt = lax.axis_index("tensor")
            for a in range(C):
                for b in range(F):
                    dest = (mf ^ b) * C + (mc ^ mask_of(a, C, mt))
                    w[at(dest * rows, rows, rows), :] = wb[a // CH][a % CH, b]
            for b in range(2 * F):
                dy[b * half : (b + 1) * half, :] = db[b // FH][b % FH]
            du[...] = mm(dy[...], w[:, 2 * hp :])

        w_f, dy, du = call(
            ffn_pre,
            [shape(width, 3 * hp), shape(R, width), shape(R, hp, dtype=F32)],
            wf + dys,
            flops=2 * R * width * hp,
        )

        h2s = spread(h2s, "fsdp", F, 1, late=du)

        def ffn_main(*refs):
            hb, w, du_ref, own, low, high, h2, act = refs[: 2 * F], *refs[2 * F :]
            for b in range(2 * F):
                h2[b * half : (b + 1) * half, :] = hb[b][...]
            p = mm(h2[...], w[:, : 2 * hp])
            gate, up = p[:, :hp], p[:, hp:]
            sg = 1.0 / (1.0 + jnp.exp(-gate))
            d = du_ref[...]
            sl = gate * sg
            act[:, :hp] = (d * up * sg * (1.0 + gate * (1.0 - sg))).astype(BF)
            act[:, hp : 2 * hp] = (d * sl).astype(BF)
            act[:, 2 * hp :] = (sl * up).astype(BF)
            split_rows(mm_t(act[:, : 2 * hp], w[:, : 2 * hp]), own, low, high)

        res = call(
            ffn_main,
            halves + [shape(R, width), shape(R, 3 * hp)],
            h2s + [w_f, du],
            flops=8 * R * width * hp,
        )
        h2, act = res[3:]
        dh2, dh2_sent = reduce(*res[:3], "fsdp", F)
        act = after(act, dh2_sent)

        def ffn_post(h2_ref, dy_ref, act_ref, w, *refs):
            own, send, gd, gu, g = refs[0], refs[1], refs[2:4], refs[4:6], refs[6]
            mf, mc = me()
            mt = lax.axis_index("tensor")
            g[:, : 2 * hp] = mt_m(h2_ref[...], act_ref[:, : 2 * hp]).astype(BF)
            g[:, 2 * hp :] = mt_m(dy_ref[...], act_ref[:, 2 * hp :]).astype(BF)
            for a in range(C):
                for b in range(F):
                    dest = (mf ^ b) * C + (mc ^ mask_of(a, C, mt))
                    src = at(dest * rows, rows, rows)
                    gu[a // CH][a % CH, b] = g[src, : 2 * hp]
                    gd[a // CH][a % CH, b] = g[src, 2 * hp :]
            split_whole(mm_t(act_ref[:, 2 * hp :], w[:, 2 * hp :]), own, send)

        res = call(
            ffn_post,
            whole + [shape(CH, F, rows, hp)] * 2 + [shape(CH, F, rows, 2 * hp)] * 2,
            [h2, dy, act, w_f],
            [pltpu.VMEM((width, 3 * hp), BF)],
            flops=8 * R * width * hp,
        )
        out_parts, down_parts, units_parts = list(res[:2]) + [None], res[2:4], res[4:6]

        inward, gn_rows = norm_back(x_mid, r2, g_ffn, dh2)
        dg_ffn = jnp.sum(gn_rows, 0, keepdims=True)
        dx_mid = my_half(cot).astype(F32) + inward
        dx_low = dx_mid.astype(BF)
        dxs = spread([dx_low], "context", C)
        units_first, out_first = [], []
        g_units = reduce_blocks(*after(units_parts, dxs[1:C]), "context", C, first=units_first)
        out = (x_mid + reduce(*out_parts, "fsdp", F, enter=dx_low, first=out_first)[0]).astype(BF)

        far = [w_o, q, ky, v, raw, h, w_qkv]

        def attn_back(*refs):
            far, refs = refs[:7], refs[7:]
            xb, db, refs = refs[:2], refs[2 : 2 + 2 * C], refs[2 + 2 * C :]
            gv_ref, gqk_ref, cs_ref, sn_ref, ok_ref, dgf, own, send = refs[:8]
            gb, dx, draw, gs_ref, ex, gn, ga = refs[8:10], *refs[10:16]
            wo_ref, q, ky, v, raw, h_ref, w = refs[16:23]
            sem = refs[23]
            loads = [pltpu.make_async_copy(a, b, sem.at[m]) for m, (a, b) in enumerate(zip(far, refs[16:23]))]
            for cp in loads:
                cp.start()
            for b in range(2 * C):
                dx[b * half : (b + 1) * half, :] = db[b][...]
            loads[0].wait()
            ga[...] = mm(dx[...], wo_ref[...])
            for cp in loads[1:5]:
                cp.wait()
            mf, mc = me()
            mt = lax.axis_index("tensor")
            cs, sn = cs_ref[...], sn_ref[...]
            ok = ok_ref[...].astype(F32) > 0.5
            dk, dv = [0.0] * kh, [0.0] * kh
            dgq, dgk = jnp.zeros((1, HEAD), F32), jnp.zeros((1, HEAD), F32)
            for j in range(qh):
                qs = slice(j * HEAD, (j + 1) * HEAD)
                ks = slice(j // group * HEAD, (j // group + 1) * HEAD)
                qj, kj, vj, g = q[:, qs], ky[:, ks], v[:, ks], ga[:, qs]
                e = jnp.where(ok, jnp.exp(mm_t(qj, kj) * scale), 0.0)
                inv = 1.0 / jnp.sum(e, -1, keepdims=True)
                eb = e.astype(BF)
                attn = mm(eb, vj) * inv
                gsc = (g * inv).astype(BF)
                dt = -jnp.sum(g * attn, -1, keepdims=True) * inv
                dv[j // group] += mt_m(eb, gsc)
                ds = (e * (mm_t(gsc, vj) + dt)).astype(BF)
                dk[j // group] += mt_m(ds, qj) * scale
                a = raw[:, qs]
                back, dg = norm_back(a, inv_rms(a), gqk_ref[0:1, :], rotate(mm(ds, kj) * scale, cs, -sn))
                draw[:, qs] = back.astype(BF)
                dgq += jnp.sum(dg, 0, keepdims=True)
            for j in range(kh):
                ks = slice(qc + j * HEAD, qc + (j + 1) * HEAD)
                a = raw[:, ks]
                back, dg = norm_back(a, inv_rms(a), gqk_ref[1:2, :], rotate(dk[j], cs, -sn))
                draw[:, ks] = back.astype(BF)
                dgk += jnp.sum(dg, 0, keepdims=True)
                draw[:, qc + kw + j * HEAD : qc + kw + (j + 1) * HEAD] = dv[j].astype(BF)
            for cp in loads[5:]:
                cp.wait()
            gs_ref[...] = mt_m(h_ref[...], draw[...]).astype(BF)
            dh = mm_t(draw[...], w[...])
            split_whole(dh, own, send)
            total = jnp.zeros((1, width), F32)
            for b in range(2 * C):
                x = xb[b // C][b % C * half : (b % C + 1) * half, :].astype(F32)
                total += jnp.sum(dh[b * half : (b + 1) * half] * (x * inv_rms(x)), 0, keepdims=True)
            gn[0:1, :] = total
            gn[1:2, :] = dgf[...]
            ex[...] = jnp.zeros_like(ex)
            for a in range(F):
                for b in range(C):
                    dest = (mf ^ mask_of(a, F, mt)) * C + (mc ^ b)
                    gb[a // FH][a % FH, b * rows : (b + 1) * rows, :] = gs_ref[at(dest * rows, rows, rows), :]
                    blk = at(dest * rows // 128 * 128, 128, 128)
                    ex[2 * b : 2 * b + 1, 0:128] = gn[0:1, blk]
                    ex[2 * b : 2 * b + 1, 128:256] = gn[1:2, blk]
                    ex[2 * b : 2 * b + 1, 256:384] = dgq
                    ex[2 * b + 1 : 2 * b + 2, 0:128] = dgk
                gb[a // FH][a % FH, CR:, :] = ex[...].astype(BF)

        res = call(
            attn_back,
            whole + [shape(FH, CR + 2 * C, aw)] * 2 + [shape(R, width)],
            far + xs + dxs + [gv, gqk, cos, sin, allowed, dg_ffn],
            [pltpu.VMEM((R, aw), BF), pltpu.VMEM((width, aw), BF), pltpu.VMEM((2 * C, aw), F32), pltpu.VMEM((8, width), F32), pltpu.VMEM((R, qc), F32)]
            + [pltpu.VMEM(a.shape, a.dtype) for a in far]
            + [pltpu.SemaphoreType.DMA((7,))],
            hbm=7,
            flops=2 * R * width * qc + 4 * R * width * aw + 12 * R * R * qc,
            vmem_mb=24,
        )
        g_down = reduce_blocks(*after(down_parts, dxs[1:C]), "context", C, gate=res[0])
        def out_grad(dx, o_ref, ga, gb, g):
            refs = (ga, gb)
            mf, mc = me()
            mt = lax.axis_index("tensor")
            g[...] = mt_m(dx[...], o_ref[...]).astype(BF)
            for a in range(F):
                for b in range(C):
                    dest = (mf ^ mask_of(a, F, mt)) * C + (mc ^ b)
                    refs[a // FH][a % FH, b * rows : (b + 1) * rows, :] = g[at(dest * rows, rows, rows), :]

        go = call(
            out_grad,
            [shape(FH, CR, qc)] * 2,
            [after(res[4], units_first[0]), o],
            [pltpu.VMEM((width, qc), BF)],
            flops=2 * R * width * qc,
        )
        dh, dh_sent = reduce(res[0], res[1], None, "context", C, enter=units_first[0])
        q_first = []
        gq = reduce_blocks(res[2], res[3], "fsdp", F, gate=(g_units, g_down, go[1], dh_sent), first=q_first).astype(BF)
        o_first = []
        go = reduce_blocks(go[0], go[1], "fsdp", F, first=o_first)
        gf = jnp.concatenate([g_units.astype(BF), g_down.astype(BF)], -1)
        gf = scatter([gf[0]] + list(after([gf[k] for k in range(1, F)], q_first[0], o_first[0])), "fsdp", F)

        def ffn_owner(*refs):
            b, outs = refs[:F], refs[F:]
            mf, _ = me()
            for k in range(F):
                d = at((mf ^ k) * hp, hp, 128)
                for m in range(3):
                    outs[m][:, d] = b[k][:, m * hp : (m + 1) * hp].astype(F32)

        ffn_grads = call(ffn_owner, [shape(rows, F * hp, dtype=F32)] * 3, gf)
        if hp > hc:
            ffn_grads = [g.reshape(rows, F, hp)[:, :, :hc].reshape(rows, F * hc) for g in ffn_grads]
        go = go.astype(BF)
        ga = []
        for j in range(C):
            both_grads = jnp.concatenate([gq[j * rows : (j + 1) * rows], go[j * rows : (j + 1) * rows]], 1)
            gains = jnp.pad(gq[CR + 2 * j : CR + 2 * j + 2], ((0, 6), (0, qc)))
            ga.append(jnp.concatenate([both_grads, gains], 0))
        ga = scatter([ga[0]] + list(after(ga[1:], gf[1])), "context", C)
        x32 = x_half.astype(F32)
        inward, _ = norm_back(x32, inv_rms(x32), gv[0:1], dh)
        grad_hidden = (dx_mid + inward).astype(BF)

        rows_out = [both_halves(out).reshape(1, tokens, width), both_halves(grad_hidden).reshape(1, tokens, width)]

        def attn_owner(*refs):
            b, gwq, gwk, gwv, gwo, ge = refs[:C], *refs[C:]
            _, mc = me()
            if share > 1:
                gwk[...] = jnp.zeros_like(gwk)
                gwv[...] = jnp.zeros_like(gwv)
            e = jnp.zeros((8, aw), F32)
            for j in range(C):
                d = mc ^ j
                gwq[:, at(d * qc, qc, 128)] = b[j][0:rows, :qc].astype(F32)
                gwo[:, at(d * qc, qc, 128)] = b[j][0:rows, aw:].astype(F32)
                ks = at(d * kv_local // C * HEAD, kw, 128)
                gk = b[j][0:rows, qc : qc + kw].astype(F32)
                gw = b[j][0:rows, qc + kw : aw].astype(F32)
                if share > 1:
                    gwk[:, ks] += gk
                    gwv[:, ks] += gw
                else:
                    gwk[:, ks] = gk
                    gwv[:, ks] = gw
                e += b[j][rows:, :aw].astype(F32)
            ge[...] = e

        gwq, gwk, gwv, gwo, ge = call(
            attn_owner,
            [
                shape(rows, C * qc, dtype=F32), shape(rows, kv_local * HEAD, dtype=F32),
                shape(rows, kv_local * HEAD, dtype=F32), shape(rows, C * qc, dtype=F32), shape(8, aw, dtype=F32),
            ],
            [after(ga[0], rows_out)] + ga[1:],
        )
        ge = ge + swap_t(ge)

        def piece(row, start, off, size):
            return lax.dynamic_slice(ge, (row, start + off), (1, size)).reshape(size)

        return (
            *rows_out,
            gwq, gwk, gwv, gwo.T,
            ffn_grads[0], ffn_grads[1], ffn_grads[2].T,
            piece(0, 0, lane, rows), piece(0, 128, lane, rows), piece(0, 256, goff, grow), piece(1, 0, goff, grow),
        )

    both = ("fsdp", "context")
    seq, row, col, vec = P("fsdp", "context", None), P(both, "tensor"), P("tensor", both), P(both)
    return jax.shard_map(
        local,
        mesh=mesh,
        in_specs=(seq, P("fsdp", "context"), row, row, row, col, row, row, col, vec, vec, vec, vec, seq),
        out_specs=(seq, seq, row, row, row, col, row, row, col, vec, vec, vec, vec),
        check_vma=False,
    )
```

```python
import jax
import jax.numpy as jnp
from jax import lax
from jax.experimental import pallas as pl
from jax.experimental.pallas import tpu as pltpu
from jax.sharding import PartitionSpec as P

HEAD = 128
EPS = 1e-06
THETA = 1000000.0
BF = jnp.bfloat16
F32 = jnp.float32


def mm(a, b):
    return lax.dot_general(a, b, (((1,), (0,)), ((), ())), preferred_element_type=F32)


def mm_t(a, b):
    return lax.dot_general(a, b, (((1,), (1,)), ((), ())), preferred_element_type=F32)


def mt_m(a, b):
    return lax.dot_general(a, b, (((0,), (0,)), ((), ())), preferred_element_type=F32)


def inv_rms(v):
    return lax.rsqrt(jnp.mean(v * v, axis=-1, keepdims=True) + EPS)


def norm_back(v, r, g, up):
    n = v * r
    w = up * g
    return r * (w - n * jnp.mean(w * n, axis=-1, keepdims=True)), up * n


def swap(x, axis, n, k):
    return lax.ppermute(x, axis, [(i, i ^ k) for i in range(n)])


def bits(n):
    return n.bit_length() - 1


def turned(j, n):
    return sum(((j >> i) & 1) << (bits(n) - 1 - i) for i in range(bits(n)))


def mask_of(j, n, t):
    return j + t * (turned(j, n) - j)


def hop(x, axis, n, i):
    steps = [1 << i, 1 << (bits(n) - 1 - i)]
    return lax.ppermute(x, (axis, "tensor"), [(2 * d + t, 2 * (d ^ steps[t]) + t) for d in range(n) for t in range(2)])


def scatter(blocks, axis, n):
    got = {k: swap(blocks[k], axis, n, k) for k in range(n - 1, 0, -1)}
    return [blocks[0]] + [got[k] for k in range(1, n)]


def join(a, b):
    def body(a_ref, b_ref, o_ref):
        o_ref[: a.shape[0]] = a_ref[...]
        o_ref[a.shape[0] :] = b_ref[...]

    return call(body, [shape(2 * a.shape[0], *a.shape[1:])], [a, b], vmem_mb=8)[0]


def gather(x, axis, n, gate=None, first=None):
    x = x[None]
    for i in range(bits(n)):
        got = hop(x, axis, n, i)
        if first is not None and i == 0:
            first.append(got)
        if i < bits(n) - 1:
            x = join(x, got if gate is None else after(got, gate))
    return [x, got]


def reduce_blocks(low, high, axis, n, gate=None, first=None, last=None):
    for i in range(bits(n) - 1, -1, -1):
        got = hop(high, axis, n, i)
        if first is not None and i == bits(n) - 1:
            first.append(got)
        if gate is not None and i:
            got = after(got, gate)
        if last is not None and not i:
            got = after(got, last)
        low = low.astype(F32) + got.astype(F32)
        if i:
            keep = low.shape[0] // 2
            low, high = low[:keep], low[keep:].astype(BF)
    return low[0]


def after(x, *deps):
    return lax.optimization_barrier((x, deps))[0]


def at(offset, size, unit):
    return pl.ds(pl.multiple_of(offset, unit), size)


def call(body, outs, args, scratch=(), flops=0, vmem_mb=20, hbm=0, hbm_outs=0):
    vmem = pl.BlockSpec(memory_space=pltpu.VMEM)
    far = pl.BlockSpec(memory_space=pltpu.MemorySpace.HBM)
    moved = sum(a.size * a.dtype.itemsize for a in list(args) + list(outs))
    outs = [pltpu.HBM(a.shape, a.dtype) for a in outs[:hbm_outs]] + list(outs[hbm_outs:])
    args = [pltpu.with_memory_space_constraint(a, pltpu.HBM) for a in args[:hbm]] + list(args[hbm:])
    return pl.pallas_call(
        body,
        out_shape=list(outs),
        in_specs=[far] * hbm + [vmem] * (len(args) - hbm),
        out_specs=[far] * hbm_outs + [vmem] * (len(outs) - hbm_outs),
        scratch_shapes=list(scratch),
        cost_estimate=pl.CostEstimate(flops=flops, bytes_accessed=moved, transcendentals=0),
        compiler_params=pltpu.CompilerParams(vmem_limit_bytes=vmem_mb * 1024 * 1024),
    )(*args)


def shape(*s, dtype=BF):
    return jax.ShapeDtypeStruct(s, dtype)


def solution(mesh):
    F, C, T = mesh.shape["fsdp"], mesh.shape["context"], mesh.shape["tensor"]

    def local(
        hidden, segments, w_query, w_key, w_value, w_out, w_gate, w_up, w_down,
        gain_attn, gain_ffn, gain_query, gain_key, cotangent,
    ):
        f, c, t = lax.axis_index("fsdp"), lax.axis_index("context"), lax.axis_index("tensor")
        tokens, width = hidden.shape[1], hidden.shape[2]
        half = tokens // T
        rows = w_query.shape[0]
        grow = gain_query.shape[0]
        kv_local = w_key.shape[1] // HEAD
        qc = w_query.shape[1] // C
        kw = max(HEAD, w_key.shape[1] // C)
        hc = w_gate.shape[1] // F
        hp = -(-hc // 128) * 128
        qh, kh = qc // HEAD, kw // HEAD
        group = qh // kh
        aw = qc + 2 * kw
        CR = C * rows
        R = T * C * half
        H = R // 2
        scale = HEAD ** (-0.5)
        share = kw * C // w_key.shape[1]
        wide = aw + qc + width
        CH, FH = C // 2, F // 2

        lane = (f * C + c) * rows % 128
        goff = (f * C + c) * grow

        hid = hidden.reshape(tokens, width)
        tall = max(rows, half)

        def me():
            return lax.axis_index("fsdp"), lax.axis_index("context")

        def ffn_pack(wg_ref, wu_ref, wd_ref, *refs):
            outs, sem = refs[:F], refs[F]
            mf, _ = me()
            copies = []
            for k in range(F):
                for j, w in enumerate((wg_ref, wu_ref, wd_ref)):
                    copies.append(pltpu.make_async_copy(w.at[:, at((mf ^ k) * hp, hp, 128)], outs[k].at[:, j * hp : (j + 1) * hp], sem.at[k, j]))
            for cp in copies:
                cp.start()
            for cp in copies:
                cp.wait()

        w_down = w_down.T
        if hp > hc:
            fill = [((0, 0), (0, 0), (0, hp - hc))]
            w_gate, w_up, w_down = [jnp.pad(w.reshape(rows, F, hc), *fill).reshape(rows, F * hp) for w in (w_gate, w_up, w_down)]
        def attn_pack(wq_ref, wk_ref, wv_ref, wo_ref, x_ref, ga_ref, gf_ref, gq_ref, gk_ref, s_ref, *refs):
            outs, sem, small = refs[:C], refs[C], refs[C + 1 : C + 6]
            mt = lax.axis_index("tensor")
            mf, mc = me()
            given = (ga_ref, gf_ref, gq_ref, gk_ref, s_ref)
            early = [pltpu.make_async_copy(a, b, sem.at[0, 5 + m]) for m, (a, b) in enumerate(zip(given, small))]
            for cp in early:
                cp.start()
            ga_ref, gf_ref, gq_ref, gk_ref, s_ref = small
            copies = []
            for k in range(C):
                d = mc ^ k
                ks = at(d * kv_local // C * HEAD, kw, 128)
                qs = at(d * qc, qc, 128)
                parts = [(wq_ref, qs, 0, qc), (wk_ref, ks, qc, kw), (wv_ref, ks, qc + kw, kw), (wo_ref, qs, aw, qc)]
                copies.append(pltpu.make_async_copy(x_ref.at[at(mt * half, half, half), :], outs[k].at[0:half, aw + qc :], sem.at[k, 4]))
                for m, (w, src, start, size) in enumerate(parts):
                    copies.append(pltpu.make_async_copy(w.at[:, src], outs[k].at[0:rows, start : start + size], sem.at[k, m]))
            for cp in copies:
                cp.start()
            for cp in early:
                cp.wait()
            dest = mf * C + mc
            lanes = lax.broadcasted_iota(jnp.int32, (8, 128), 1)
            docs = jnp.broadcast_to(s_ref[...].astype(F32), (8, 128))
            docs = jnp.where((lanes < half) == (mt == 0), docs, pltpu.roll(docs, half, 1))

            def placed(ref, want):
                size = ref.shape[1]
                r = lax.broadcasted_iota(jnp.int32, (size, 128), 0)
                pick = (lax.broadcasted_iota(jnp.int32, (size, 128), 1) == r + want).astype(F32).astype(BF)
                return mm(jnp.broadcast_to(ref[...].astype(F32), (8, size)).astype(BF), pick)[0:1]

            ln, hd = dest * rows % 128, dest * grow
            blank = jnp.zeros((1, aw - 384), F32) if aw > 384 else None
            first = [placed(ga_ref, ln), placed(gf_ref, ln), placed(gq_ref, hd)]
            first = jnp.concatenate(first + ([blank] if aw > 384 else []), 1)
            second = jnp.concatenate([placed(gk_ref, hd), jnp.zeros((1, aw - 128), F32)], 1)
            ext = jnp.concatenate([first, second, jnp.zeros((6, aw), F32)], 0).astype(BF)
            for k in range(C):
                outs[k][tall:, :aw] = ext
                outs[k][tall:, aw : aw + qc] = jnp.zeros((8, qc), BF)
                outs[k][tall:, aw + qc : aw + qc + 128] = docs.astype(BF)
                outs[k][tall:, aw + qc + 128 :] = jnp.zeros((8, width - 128), BF)
            for cp in copies:
                cp.wait()

        wa = call(
            attn_pack,
            [shape(tall + 8, wide)] * C,
            [w_query, w_key, w_value, w_out.T, hid]
            + [v.reshape(1, -1) for v in (gain_attn, gain_ffn, gain_query, gain_key)]
            + [segments.reshape(1, tokens)],
            [pltpu.SemaphoreType.DMA((C, 10))]
            + [pltpu.VMEM((1, v.shape[0]), BF) for v in (gain_attn, gain_ffn, gain_query, gain_key)]
            + [pltpu.VMEM((1, tokens), jnp.int32)],
            hbm=10,
            vmem_mb=16,
        )

        wf = call(
            ffn_pack,
            [shape(rows, 3 * hp)] * F,
            list(after((w_gate, w_up, w_down), wa[0])),
            [pltpu.SemaphoreType.DMA((F, 3))],
            hbm=3,
            vmem_mb=16,
        )
        wa_got = scatter(wa, "context", C)

        wf = scatter(wf, "fsdp", F)

        def attn_join(*refs):
            b, qkv, o, x, docs = refs[:C], refs[C], refs[C + 1], refs[C + 2], refs[C + 3]
            mt = lax.axis_index("tensor")
            docs[...] = jnp.zeros_like(docs)
            for k in range(C):
                j = mask_of(k, C, mt)
                qkv[k * rows : (k + 1) * rows, :] = b[k][0:rows, :aw]
                o[k * rows : (k + 1) * rows, :] = b[k][0:rows, aw : aw + qc]
                x[at(j * half, half, half), :] = b[k][0:half, aw + qc :]
                docs[pl.ds(j, 1), :] = b[k][tall:, aw + qc : aw + qc + 128].astype(F32)[0:1]
            x[C * half :, :128] = docs[...].astype(BF)
            x[C * half :, 128:] = jnp.zeros((8, width - 128), BF)
            qkv[CR:, :] = jnp.concatenate([b[k][tall:, :aw].astype(F32)[0:2] for k in range(C)], 0).astype(BF)

        wq, wo, x_own = call(
            attn_join,
            [shape(CR + 2 * C, aw), shape(CR, qc), shape(C * half + 8, width)],
            [after(wa_got[0], wf[1], wf[F - 1])] + wa_got[1:],
            [pltpu.VMEM((8, 128), F32)],
        )
        q_here = []
        wq = gather(wq, "fsdp", F, first=q_here)
        wo = gather(after(wo, wq[0]), "fsdp", F)

        def ffn_join(*refs):
            for k in range(F):
                refs[F][k] = refs[k][...]

        wf_got = wf
        wf = call(ffn_join, [shape(F, rows, 3 * hp)], [after(wf[0], q_here[0])] + wf[1:], vmem_mb=8)[0]
        wf_first = hop(wf[None], "context", C, 0)
        wf_here = wf[None]

        def my_half(x):
            return lax.dynamic_slice_in_dim(x, t * half, half, 0)

        def other_half(x):
            return lax.dynamic_slice_in_dim(x, (1 - t) * half, half, 0)

        def swap_t(x):
            return swap(x, "tensor", T, 1)

        x_half = my_half(hid)
        xs = [x_own, swap_t(x_own)]

        idx = jnp.arange(R, dtype=jnp.int32)
        trel, k, i = idx // (C * half), (idx // half) % C, idx % half
        pos = (c ^ mask_of(k, C, t ^ trel)) * tokens + (t ^ trel) * half + i
        freq = THETA ** (-(jnp.arange(HEAD // 2, dtype=F32) * 2.0 / HEAD))
        angle = pos.astype(F32)[:, None] * freq[None, :]
        cos, sin = jnp.cos(angle), jnp.sin(angle)
        cos, sin = jnp.concatenate([cos, cos], 1), jnp.concatenate([-sin, sin], 1)
        pos_row = jnp.broadcast_to(pos[None], (8, R))
        pos_col = jnp.broadcast_to(pos[:, None], (R, 128))

        def find_allowed(a_ref, b_ref, pr_ref, pc_ref, out):
            copies = CH * (2 * half // 128)
            row = []
            for ref in (a_ref, b_ref):
                d = ref[C * half :, :128].astype(F32)
                d = jnp.concatenate([d] * (C * half // 128), 1)
                keep = lax.broadcasted_iota(jnp.int32, d.shape, 1) // half == lax.broadcasted_iota(jnp.int32, d.shape, 0)
                row.append(jnp.sum(jnp.where(keep, d, 0.0), 0, keepdims=True))
            row = jnp.broadcast_to(jnp.concatenate(row, 1), (8, R))
            first = (lax.broadcasted_iota(jnp.int32, (8, 128), 0) == 0).astype(F32).astype(BF)
            col = mt_m(row.astype(BF), first)
            pc = pc_ref[...]
            for m in range(R // 128):
                sl = slice(m * 128, (m + 1) * 128)
                ok = (col == row[0:1, sl]) & (pc >= pr_ref[0:1, sl])
                out[:, sl] = jnp.where(ok, 1.0, 0.0).astype(BF)

        allowed = call(find_allowed, [shape(R, R)], xs + [pos_row, pos_col])[0]

        def pair_sum(own, low, high, enter=None):
            keep = H // 2
            if high is None:
                low = swap_t(low)
                low, high = low[:keep], low[keep:]
            else:
                low, high = swap_t(low), swap_t(high)
            high = (own[keep:] + high.astype(F32)).astype(BF)
            low = own[:keep] + low.astype(F32)
            if enter is not None:
                high = after(high, enter)
            return low, high

        def finish(low, high, axis, n, first=None, last=None):
            shaped = (n // 2, half, width)
            return reduce_blocks(low.reshape(shaped), high.reshape(shaped), axis, n, None, first, last)

        def reduce(own, low, high, axis, n, enter=None, first=None, last=None):
            low, high = pair_sum(own, low, high, enter)
            return finish(low, high, axis, n, first, last), high

        def spread(b, axis, n, start=0, late=None):
            for i in range(start, bits(n)):
                b = b + [hop(a, axis, n, i) for a in b]
            last = b[-1] if late is None else after(b[-1], late)
            return b + [swap_t(a) for a in b[:-1] + [last]]

        def both_halves(x):
            y = swap_t(x)
            return jnp.where(t == 0, jnp.concatenate([x, y], 0), jnp.concatenate([y, x], 0))

        cot = cotangent.reshape(tokens, width)
        def rotate(v, cs, sn):
            return v * cs + pltpu.roll(v, HEAD // 2, 1) * sn

        def split_rows(p, own, low, high):
            own[...] = p[:H]
            low[...] = p[H : H + H // 2].astype(BF)
            high[...] = p[H + H // 2 :].astype(BF)

        def split_whole(p, own, send):
            own[...] = p[:H]
            send[...] = p[H:].astype(BF)

        whole = [shape(H, width, dtype=F32), shape(H, width)]
        halves = [shape(H, width, dtype=F32), shape(H // 2, width), shape(H // 2, width)]

        got = after(wf_first, wo[0])
        for i in range(1, bits(C)):
            wf_here = join(wf_here, got)
            got = hop(wf_here, "context", C, i)
        wf = [wf_here, got]

        def attn_fwd(*refs):
            xb, wb, refs = refs[:2], refs[2:4], refs[4:]
            cs_ref, sn_ref, ok_ref = refs[:3]
            outs, o, gv, gqk = refs[3:9], refs[9], refs[10], refs[11]
            h, raw, q, ky, v, w = refs[12:18]
            sem = refs[18]
            mf, mc = me()
            mt = lax.axis_index("tensor")
            sent = [pltpu.make_async_copy(a, b, sem.at[m]) for m, (a, b) in enumerate(zip((h, raw, q, ky, v, w), outs))]
            gv[...] = jnp.zeros_like(gv)
            acc = jnp.zeros((2, 128), F32)
            for a in range(F):
                wa_ref = wb[a // FH]
                e = wa_ref[a % FH, CR:, :].astype(F32)
                for b in range(C):
                    dest = (mf ^ mask_of(a, F, mt)) * C + (mc ^ b)
                    w[at(dest * rows, rows, rows), :] = wa_ref[a % FH, b * rows : (b + 1) * rows, :]
                    blk = at(dest * rows // 128 * 128, 128, 128)
                    gv[0:1, blk] += e[2 * b : 2 * b + 1, 0:128]
                    gv[1:2, blk] += e[2 * b : 2 * b + 1, 128:256]
                    acc += jnp.concatenate([e[2 * b : 2 * b + 1, 256:384], e[2 * b + 1 : 2 * b + 2, 0:128]], 0)
            gqk[0:2, :] = acc
            g = gv[0:1, :]
            for b in range(2 * C):
                x = xb[b // C][b % C * half : (b % C + 1) * half, :].astype(F32)
                h[b * half : (b + 1) * half, :] = (x * inv_rms(x) * g).astype(BF)
            sent[0].start()
            sent[5].start()
            p = mm(h[...], w[...])
            raw[...] = p[:, : qc + kw]
            v[...] = p[:, qc + kw :].astype(BF)
            sent[1].start()
            sent[4].start()
            cs, sn = cs_ref[...], sn_ref[...]
            for j in range(qh + kh):
                a = p[:, j * HEAD : (j + 1) * HEAD]
                gg = gqk[0:1, :] if j < qh else gqk[1:2, :]
                rot = rotate(a * inv_rms(a) * gg, cs, sn).astype(BF)
                if j < qh:
                    q[:, j * HEAD : (j + 1) * HEAD] = rot
                else:
                    ky[:, (j - qh) * HEAD : (j - qh + 1) * HEAD] = rot
            sent[2].start()
            sent[3].start()
            ok = ok_ref[...].astype(F32) > 0.5
            for j in range(qh):
                qs = slice(j * HEAD, (j + 1) * HEAD)
                ks = slice(j // group * HEAD, (j // group + 1) * HEAD)
                e = jnp.where(ok, jnp.exp(mm_t(q[:, qs], ky[:, ks]) * scale), 0.0)
                o[:, qs] = (mm(e.astype(BF), v[:, ks]) / jnp.sum(e, -1, keepdims=True)).astype(BF)
            for cp in sent:
                cp.wait()

        kept = [shape(R, width), shape(R, qc + kw, dtype=F32), shape(R, qc), shape(R, kw), shape(R, kw), shape(width, aw)]
        h, raw, q, ky, v, w_qkv, o, gv, gqk = call(
            attn_fwd,
            kept + [shape(R, qc), shape(8, width, dtype=F32), shape(8, 128, dtype=F32)],
            xs + wq + [cos, sin, after(allowed, wf_first, wo[0])],
            [pltpu.VMEM(a.shape, a.dtype) for a in kept] + [pltpu.SemaphoreType.DMA((6,))],
            flops=2 * R * width * aw + 4 * R * R * qc,
            hbm_outs=6,
        )

        def out_proj(o_ref, *refs):
            wb, w_far, o_far, own, low, high, w, sem = refs[:2], *refs[2:]
            mf, mc = me()
            mt = lax.axis_index("tensor")
            kept = [pltpu.make_async_copy(o_ref, o_far, sem.at[0]), pltpu.make_async_copy(w, w_far, sem.at[1])]
            kept[0].start()
            for a in range(F):
                for b in range(C):
                    dest = (mf ^ mask_of(a, F, mt)) * C + (mc ^ b)
                    w[at(dest * rows, rows, rows), :] = wb[a // FH][a % FH, b * rows : (b + 1) * rows, :]
            kept[1].start()
            split_rows(mm_t(o_ref[...], w[...]), own, low, high)
            for cp in kept:
                cp.wait()

        res = call(
            out_proj,
            [shape(width, qc), shape(R, qc)] + halves,
            [o] + wo,
            [pltpu.VMEM((width, qc), BF), pltpu.SemaphoreType.DMA((2,))],
            hbm_outs=2,
            flops=2 * R * width * qc,
        )
        w_o, o = res[:2]
        low, high = pair_sum(*res[2:])
        branch_first = []
        x_mid = x_half.astype(F32) + finish(low, high, "context", C, first=branch_first)
        dys = gather(after(my_half(cot), gv), "fsdp", F, gate=branch_first[0])
        r2 = inv_rms(x_mid)
        g_ffn = gv[1:2]
        h2s = [(x_mid * r2 * g_ffn).astype(BF)]
        h2s = h2s + [hop(h2s[0], "fsdp", F, 0)]
        dys = dys + [swap_t(dys[0]), swap_t(after(dys[1], h2s[1]))]

        def ffn_pre(*refs):
            wb, db, w, dy, du = refs[:2], refs[2:6], *refs[6:]
            mf, mc = me()
            mt = lax.axis_index("tensor")
            for a in range(C):
                for b in range(F):
                    dest = (mf ^ b) * C + (mc ^ mask_of(a, C, mt))
                    w[at(dest * rows, rows, rows), :] = wb[a // CH][a % CH, b]
            for b in range(2 * F):
                dy[b * half : (b + 1) * half, :] = db[b // FH][b % FH]
            du[...] = mm(dy[...], w[:, 2 * hp :])

        w_f, dy, du = call(
            ffn_pre,
            [shape(width, 3 * hp), shape(R, width), shape(R, hp, dtype=F32)],
            wf + dys,
            flops=2 * R * width * hp,
        )

        h2s = spread(h2s, "fsdp", F, 1, late=du)

        def ffn_main(*refs):
            hb, w, du_ref, own, low, high, h2, act = refs[: 2 * F], *refs[2 * F :]
            for b in range(2 * F):
                h2[b * half : (b + 1) * half, :] = hb[b][...]
            p = mm(h2[...], w[:, : 2 * hp])
            gate, up = p[:, :hp], p[:, hp:]
            sg = 1.0 / (1.0 + jnp.exp(-gate))
            d = du_ref[...]
            sl = gate * sg
            act[:, :hp] = (d * up * sg * (1.0 + gate * (1.0 - sg))).astype(BF)
            act[:, hp : 2 * hp] = (d * sl).astype(BF)
            act[:, 2 * hp :] = (sl * up).astype(BF)
            split_rows(mm_t(act[:, : 2 * hp], w[:, : 2 * hp]), own, low, high)

        res = call(
            ffn_main,
            halves + [shape(R, width), shape(R, 3 * hp)],
            h2s + [w_f, du],
            flops=8 * R * width * hp,
        )
        h2, act = res[3:]
        dh2, dh2_sent = reduce(*res[:3], "fsdp", F)
        act = after(act, dh2_sent)

        def ffn_post(h2_ref, dy_ref, act_ref, w, *refs):
            own, send, gd, gu, g = refs[0], refs[1], refs[2:4], refs[4:6], refs[6]
            mf, mc = me()
            mt = lax.axis_index("tensor")
            g[:, : 2 * hp] = mt_m(h2_ref[...], act_ref[:, : 2 * hp]).astype(BF)
            g[:, 2 * hp :] = mt_m(dy_ref[...], act_ref[:, 2 * hp :]).astype(BF)
            for a in range(C):
                for b in range(F):
                    dest = (mf ^ b) * C + (mc ^ mask_of(a, C, mt))
                    src = at(dest * rows, rows, rows)
                    gu[a // CH][a % CH, b] = g[src, : 2 * hp]
                    gd[a // CH][a % CH, b] = g[src, 2 * hp :]
            split_whole(mm_t(act_ref[:, 2 * hp :], w[:, 2 * hp :]), own, send)

        res = call(
            ffn_post,
            whole + [shape(CH, F, rows, hp)] * 2 + [shape(CH, F, rows, 2 * hp)] * 2,
            [h2, dy, act, w_f],
            [pltpu.VMEM((width, 3 * hp), BF)],
            flops=8 * R * width * hp,
        )
        out_parts, down_parts, units_parts = list(res[:2]) + [None], res[2:4], res[4:6]

        inward, gn_rows = norm_back(x_mid, r2, g_ffn, dh2)
        dg_ffn = jnp.sum(gn_rows, 0, keepdims=True)
        dx_mid = my_half(cot).astype(F32) + inward
        dx_low = dx_mid.astype(BF)
        dxs = spread([dx_low], "context", C)
        units_first, out_first = [], []
        g_units = reduce_blocks(*after(units_parts, dxs[1:C]), "context", C, first=units_first)
        out = (x_mid + reduce(*out_parts, "fsdp", F, enter=dx_low, first=out_first)[0]).astype(BF)

        far = [w_o, q, ky, v, raw, h, w_qkv]

        def attn_back(*refs):
            far, refs = refs[:7], refs[7:]
            xb, db, refs = refs[:2], refs[2 : 2 + 2 * C], refs[2 + 2 * C :]
            gv_ref, gqk_ref, cs_ref, sn_ref, ok_ref, dgf, own, send = refs[:8]
            gb, dx, draw, gs_ref, ex, gn, ga = refs[8:10], *refs[10:16]
            wo_ref, q, ky, v, raw, h_ref, w = refs[16:23]
            sem = refs[23]
            loads = [pltpu.make_async_copy(a, b, sem.at[m]) for m, (a, b) in enumerate(zip(far, refs[16:23]))]
            for cp in loads:
                cp.start()
            for b in range(2 * C):
                dx[b * half : (b + 1) * half, :] = db[b][...]
            loads[0].wait()
            ga[...] = mm(dx[...], wo_ref[...])
            for cp in loads[1:5]:
                cp.wait()
            mf, mc = me()
            mt = lax.axis_index("tensor")
            cs, sn = cs_ref[...], sn_ref[...]
            ok = ok_ref[...].astype(F32) > 0.5
            dk, dv = [0.0] * kh, [0.0] * kh
            dgq, dgk = jnp.zeros((1, HEAD), F32), jnp.zeros((1, HEAD), F32)
            for j in range(qh):
                qs = slice(j * HEAD, (j + 1) * HEAD)
                ks = slice(j // group * HEAD, (j // group + 1) * HEAD)
                qj, kj, vj, g = q[:, qs], ky[:, ks], v[:, ks], ga[:, qs]
                e = jnp.where(ok, jnp.exp(mm_t(qj, kj) * scale), 0.0)
                inv = 1.0 / jnp.sum(e, -1, keepdims=True)
                eb = e.astype(BF)
                attn = mm(eb, vj) * inv
                gsc = (g * inv).astype(BF)
                dt = -jnp.sum(g * attn, -1, keepdims=True) * inv
                dv[j // group] += mt_m(eb, gsc)
                ds = (e * (mm_t(gsc, vj) + dt)).astype(BF)
                dk[j // group] += mt_m(ds, qj) * scale
                a = raw[:, qs]
                back, dg = norm_back(a, inv_rms(a), gqk_ref[0:1, :], rotate(mm(ds, kj) * scale, cs, -sn))
                draw[:, qs] = back.astype(BF)
                dgq += jnp.sum(dg, 0, keepdims=True)
            for j in range(kh):
                ks = slice(qc + j * HEAD, qc + (j + 1) * HEAD)
                a = raw[:, ks]
                back, dg = norm_back(a, inv_rms(a), gqk_ref[1:2, :], rotate(dk[j], cs, -sn))
                draw[:, ks] = back.astype(BF)
                dgk += jnp.sum(dg, 0, keepdims=True)
                draw[:, qc + kw + j * HEAD : qc + kw + (j + 1) * HEAD] = dv[j].astype(BF)
            for cp in loads[5:]:
                cp.wait()
            gs_ref[...] = mt_m(h_ref[...], draw[...]).astype(BF)
            dh = mm_t(draw[...], w[...])
            split_whole(dh, own, send)
            total = jnp.zeros((1, width), F32)
            for b in range(2 * C):
                x = xb[b // C][b % C * half : (b % C + 1) * half, :].astype(F32)
                total += jnp.sum(dh[b * half : (b + 1) * half] * (x * inv_rms(x)), 0, keepdims=True)
            gn[0:1, :] = total
            gn[1:2, :] = dgf[...]
            ex[...] = jnp.zeros_like(ex)
            for a in range(F):
                for b in range(C):
                    dest = (mf ^ mask_of(a, F, mt)) * C + (mc ^ b)
                    gb[a // FH][a % FH, b * rows : (b + 1) * rows, :] = gs_ref[at(dest * rows, rows, rows), :]
                    blk = at(dest * rows // 128 * 128, 128, 128)
                    ex[2 * b : 2 * b + 1, 0:128] = gn[0:1, blk]
                    ex[2 * b : 2 * b + 1, 128:256] = gn[1:2, blk]
                    ex[2 * b : 2 * b + 1, 256:384] = dgq
                    ex[2 * b + 1 : 2 * b + 2, 0:128] = dgk
                gb[a // FH][a % FH, CR:, :] = ex[...].astype(BF)

        res = call(
            attn_back,
            whole + [shape(FH, CR + 2 * C, aw)] * 2 + [shape(R, width)],
            far + xs + dxs + [gv, gqk, cos, sin, allowed, dg_ffn],
            [pltpu.VMEM((R, aw), BF), pltpu.VMEM((width, aw), BF), pltpu.VMEM((2 * C, aw), F32), pltpu.VMEM((8, width), F32), pltpu.VMEM((R, qc), F32)]
            + [pltpu.VMEM(a.shape, a.dtype) for a in far]
            + [pltpu.SemaphoreType.DMA((7,))],
            hbm=7,
            flops=2 * R * width * qc + 4 * R * width * aw + 12 * R * R * qc,
            vmem_mb=24,
        )
        g_down = reduce_blocks(*after(down_parts, dxs[1:C]), "context", C, gate=res[0])
        def out_grad(dx, o_ref, ga, gb, g):
            refs = (ga, gb)
            mf, mc = me()
            mt = lax.axis_index("tensor")
            g[...] = mt_m(dx[...], o_ref[...]).astype(BF)
            for a in range(F):
                for b in range(C):
                    dest = (mf ^ mask_of(a, F, mt)) * C + (mc ^ b)
                    refs[a // FH][a % FH, b * rows : (b + 1) * rows, :] = g[at(dest * rows, rows, rows), :]

        go = call(
            out_grad,
            [shape(FH, CR, qc)] * 2,
            [after(res[4], units_first[0]), o],
            [pltpu.VMEM((width, qc), BF)],
            flops=2 * R * width * qc,
        )
        dh, dh_sent = reduce(res[0], res[1], None, "context", C, enter=units_first[0])
        q_first = []
        gq = reduce_blocks(res[2], res[3], "fsdp", F, gate=(g_units, g_down, go[1], dh_sent), first=q_first).astype(BF)
        o_first = []
        go = reduce_blocks(go[0], go[1], "fsdp", F, first=o_first)
        gf = jnp.concatenate([g_units.astype(BF), g_down.astype(BF)], -1)
        gf = scatter([gf[0]] + list(after([gf[k] for k in range(1, F)], q_first[0], o_first[0])), "fsdp", F)

        def ffn_owner(*refs):
            b, outs = refs[:F], refs[F:]
            mf, _ = me()
            for k in range(F):
                d = at((mf ^ k) * hp, hp, 128)
                for m in range(3):
                    outs[m][:, d] = b[k][:, m * hp : (m + 1) * hp].astype(F32)

        ffn_grads = call(ffn_owner, [shape(rows, F * hp, dtype=F32)] * 3, gf)
        if hp > hc:
            ffn_grads = [g.reshape(rows, F, hp)[:, :, :hc].reshape(rows, F * hc) for g in ffn_grads]
        go = go.astype(BF)
        ga = []
        for j in range(C):
            both_grads = jnp.concatenate([gq[j * rows : (j + 1) * rows], go[j * rows : (j + 1) * rows]], 1)
            gains = jnp.pad(gq[CR + 2 * j : CR + 2 * j + 2], ((0, 6), (0, qc)))
            ga.append(jnp.concatenate([both_grads, gains], 0))
        ga = scatter([ga[0]] + list(after(ga[1:], gf[1])), "context", C)
        x32 = x_half.astype(F32)
        inward, _ = norm_back(x32, inv_rms(x32), gv[0:1], dh)
        grad_hidden = (dx_mid + inward).astype(BF)

        rows_out = [both_halves(out).reshape(1, tokens, width), both_halves(grad_hidden).reshape(1, tokens, width)]

        def gain_sum(*refs):
            refs[C][...] = sum([refs[j][rows:, :aw].astype(F32) for j in range(C)])

        ge = call(gain_sum, [shape(8, aw, dtype=F32)], [after(ga[0], rows_out)] + ga[1:])[0]

        def attn_owner(*refs):
            b, gwq, gwk, gwv, gwo = refs[:C], *refs[C:]
            _, mc = me()
            if share > 1:
                gwk[...] = jnp.zeros_like(gwk)
                gwv[...] = jnp.zeros_like(gwv)
            for j in range(C):
                d = mc ^ j
                gwq[:, at(d * qc, qc, 128)] = b[j][0:rows, :qc].astype(F32)
                gwo[:, at(d * qc, qc, 128)] = b[j][0:rows, aw:].astype(F32)
                ks = at(d * kv_local // C * HEAD, kw, 128)
                gk = b[j][0:rows, qc : qc + kw].astype(F32)
                gw = b[j][0:rows, qc + kw : aw].astype(F32)
                if share > 1:
                    gwk[:, ks] += gk
                    gwv[:, ks] += gw
                else:
                    gwk[:, ks] = gk
                    gwv[:, ks] = gw

        gwq, gwk, gwv, gwo = call(
            attn_owner,
            [
                shape(rows, C * qc, dtype=F32), shape(rows, kv_local * HEAD, dtype=F32),
                shape(rows, kv_local * HEAD, dtype=F32), shape(rows, C * qc, dtype=F32),
            ],
            [after(ga[0], rows_out, ge)] + ga[1:],
        )
        ge = ge + swap_t(ge)

        def piece(row, start, off, size):
            return lax.dynamic_slice(ge, (row, start + off), (1, size)).reshape(size)

        return (
            *rows_out,
            gwq, gwk, gwv, gwo.T,
            ffn_grads[0], ffn_grads[1], ffn_grads[2].T,
            piece(0, 0, lane, rows), piece(0, 128, lane, rows), piece(0, 256, goff, grow), piece(1, 0, goff, grow),
        )

    both = ("fsdp", "context")
    seq, row, col, vec = P("fsdp", "context", None), P(both, "tensor"), P("tensor", both), P(both)
    return jax.shard_map(
        local,
        mesh=mesh,
        in_specs=(seq, P("fsdp", "context"), row, row, row, col, row, row, col, vec, vec, vec, vec, seq),
        out_specs=(seq, seq, row, row, row, col, row, row, col, vec, vec, vec, vec),
        check_vma=False,
    )
```
